32 devices in a mesh: aa: 2 (over x), ba: 4 (over y, core), col: 4 (over z).
Axes of the slice: x: 2, y: 2, z: 4, core: 2. Of those that a mesh axis runs over, the one named last changes fastest.
Arguments:
- r_rows: bfloat16 [4096, 128], P(('aa', 'ba', 'col')), may hold values from -6 to 6
- r_keys: int32 [4096], P(('aa', 'ba', 'col')), may hold values from 0 to 4095
- r_counts: int32 [256], P(('aa', 'ba', 'col')), may hold values from 0 to 16, as said below
- s_rows: bfloat16 [8192, 128], P(('aa', 'ba', 'col')), may hold values from -6 to 6
- s_keys: int32 [8192], P(('aa', 'ba', 'col')), may hold values from 0 to 4095
- s_counts: int32 [512], P(('aa', 'ba', 'col')), may hold values from 0 to 16, as said below
- t_rows: bfloat16 [4096, 128], P(('aa', 'ba', 'col')), may hold values from -6 to 6
- t_keys: int32 [4096], P(('aa', 'ba', 'col')), may hold values from 0 to 4095
- t_counts: int32 [256], P(('aa', 'ba', 'col')), may hold values from 0 to 16, as said below
Outputs:
- joined: bfloat16 [4096, 128], P(('aa', 'ba', 'col'))
The draws below stay inside these ranges and needn't reach their ends.
Inputs may be any that keep to these rules, and one draw needn't show every extreme that they name: `r_counts`: in every draw one destination pair, drawn from the seed, gets 16 live slots from every device. `s_counts`: in every draw one destination pair, drawn from the seed, gets 16 live slots from every device. `t_counts`: in every draw one destination pair, drawn from the seed, gets 16 live slots from every device.
All inputs are finite; a program needn't handle non-finite values.
Results may differ from the reference program's by a relative error of at most 0.001.
Values may be sent and summed in bfloat16 or wider, within the bound.
No kernel may reach another device: no remote copies, remote signals or barrier semaphores. Data moves between devices by JAX's collectives and lax.ppermute only.
A program may use at most 64 MiB of HBM per device.

```python
import jax
import jax.numpy as jnp
from jax import lax

W = 128
KEYS = 64
CAP = 16
GROUPS_R = 8
GROUPS_S = 16
GROUPS_T = 8
N_AA = 2
N_BA = 4
N_COL = 4
DEVICES = 32


def counts_draw(key, groups):
    values = jax.random.randint(key, (DEVICES, groups), 0, CAP + 1, dtype=jnp.int32)
    heavy = jax.random.randint(jax.random.fold_in(key, 7), (), 0, groups, dtype=jnp.int32)
    column = jnp.arange(groups, dtype=jnp.int32)[None, :]
    values = jnp.where(column == heavy, CAP, values)
    return values.reshape(DEVICES * groups).astype(jnp.int32)


def draw_r_counts(key, part):
    return counts_draw(jax.random.fold_in(key, 11), GROUPS_R)


def draw_s_counts(key, part):
    return counts_draw(jax.random.fold_in(key, 13), GROUPS_S)


def draw_t_counts(key, part):
    return counts_draw(jax.random.fold_in(key, 17), GROUPS_T)


def plant(array, rng, smallest, high):
    extent = array.shape
    spot = [jax.random.randint(jax.random.fold_in(rng, axis), (), 0, extent[axis]) for axis in range(len(extent))]
    array = array.at[tuple(spot)].set(smallest)
    longest = extent.index(max(extent))
    spot[longest] = (spot[longest] + 1) % extent[longest]
    return array.at[tuple(spot)].set(high)


def block_scale(rng, extent, shards, smallest, high):
    gain, own = 1.0, jax.random.fold_in(rng, 6)
    for axis_at, blocks in shards:
        draws = jnp.exp(jax.random.uniform(jax.random.fold_in(own, axis_at), (blocks,), jnp.float32, smallest / len(shards), high / len(shards)))
        gain = gain * jnp.repeat(draws, extent[axis_at] // blocks).reshape([-1 if axis == axis_at else 1 for axis in range(len(extent))])
    return gain


def scatter_about(own_key, extent, scale, limit, pieces=(), held_as=jnp.bfloat16):
    drawn = scale * jax.random.normal(own_key, extent, jnp.float32)
    if pieces:
        drawn = drawn * block_scale(own_key, extent, pieces, -0.22, 0.18)
    return jnp.clip(drawn, -limit, limit).astype(held_as)


def setup_inputs(seed: int = 0) -> dict:
    splits = jax.random.split(jax.random.key(seed), 10)
    return {
        "r_rows": scatter_about(splits[0], (DEVICES * GROUPS_R * CAP, W), 1.0, 6.0, ((0, 32),)),
        "r_keys": plant(jax.random.randint(splits[1], (DEVICES * GROUPS_R * CAP,), 0, KEYS * KEYS), jax.random.fold_in(splits[1], 1), 0, (KEYS * KEYS) - 1).astype(jnp.int32),
        "r_counts": draw_r_counts(jax.random.fold_in(splits[9], 71), 0),
        "s_rows": scatter_about(splits[3], (DEVICES * GROUPS_S * CAP, W), 1.0, 6.0, ((0, 32),)),
        "s_keys": plant(jax.random.randint(splits[4], (DEVICES * GROUPS_S * CAP,), 0, KEYS * KEYS), jax.random.fold_in(splits[4], 1), 0, (KEYS * KEYS) - 1).astype(jnp.int32),
        "s_counts": draw_s_counts(jax.random.fold_in(splits[9], 71), 0),
        "t_rows": scatter_about(splits[6], (DEVICES * GROUPS_T * CAP, W), 1.0, 6.0, ((0, 32),)),
        "t_keys": plant(jax.random.randint(splits[7], (DEVICES * GROUPS_T * CAP,), 0, KEYS * KEYS), jax.random.fold_in(splits[7], 1), 0, (KEYS * KEYS) - 1).astype(jnp.int32),
        "t_counts": draw_t_counts(jax.random.fold_in(splits[9], 71), 0),
    }


def layout(keys, counts, first_n, second_n):
    groups = first_n * second_n
    slot = jnp.arange(keys.shape[0], dtype=jnp.int32)
    group = slot // CAP % groups
    place = slot % CAP
    live = place < counts[slot // CAP]
    first = group // second_n + first_n * (keys // KEYS)
    second = group % second_n + second_n * (keys % KEYS)
    return (first.astype(jnp.int32), second.astype(jnp.int32), live)

def reference(r_rows, r_keys, r_counts, s_rows, s_keys, s_counts, t_rows, t_keys, t_counts):
    width = r_rows.shape[1]
    key_a = KEYS * N_AA
    key_b = KEYS * N_BA
    key_c = KEYS * N_COL
    r_a, r_b, r_live = layout(r_keys, r_counts, N_AA, N_BA)
    s_b, s_c, s_live = layout(s_keys, s_counts, N_BA, N_COL)
    t_a, t_c, t_live = layout(t_keys, t_counts, N_AA, N_COL)
    s_index = (s_b * key_c + s_c).astype(jnp.int32)
    t_index = (t_a * key_c + t_c).astype(jnp.int32)
    s_weight = s_live.astype(jnp.float32)
    t_weight = t_live.astype(jnp.float32)
    sd = jax.ops.segment_sum(s_rows.astype(jnp.float32) * s_weight[:, None], s_index, key_b * key_c).reshape(key_b, key_c, width)
    scount = jax.ops.segment_sum(s_weight, s_index, key_b * key_c).reshape(key_b, key_c)
    tu = jax.ops.segment_sum(t_rows.astype(jnp.float32) * t_weight[:, None], t_index, key_a * key_c).reshape(key_a, key_c, width)
    tcount = jax.ops.segment_sum(t_weight, t_index, key_a * key_c).reshape(key_a, key_c)
    hi = lax.Precision.HIGHEST
    total = jnp.einsum('ac,bcw->abw', tcount, sd, precision=hi) + jnp.einsum('bc,acw->abw', scount, tu, precision=hi)
    triangles = jnp.einsum('ac,bc->ab', tcount, scount, precision=hi)
    flat = (r_a * key_b + r_b).astype(jnp.int32)
    gathered = total.reshape(key_a * key_b, width)[flat]
    counted = triangles.reshape(key_a * key_b)[flat]
    value = r_rows.astype(jnp.float32) * gathered / jnp.sqrt(1.0 + counted)[:, None]
    return jnp.where(r_live[:, None], value, 0.0).astype(jnp.bfloat16)
```

```python
import functools

import jax
import jax.numpy as jnp
from jax import lax
from jax.experimental import pallas as pl
from jax.experimental.pallas import tpu as pltpu
from jax.sharding import PartitionSpec as P

KEYS = 64
LANES = 128
META = 8
AXES = ("aa", "ba", "col")
f32 = jnp.float32
bf16 = jnp.bfloat16


def iota(shape, dim):
    return lax.broadcasted_iota(jnp.int32, shape, dim)


def split(x):
    hi = x.astype(bf16)
    return hi, (x - hi.astype(f32)).astype(bf16)


def mm(x, y):
    return lax.dot_general(x, y, (((1,), (0,)), ((), ())), preferred_element_type=f32)


def mm_nt(x, y):
    return lax.dot_general(x, y, (((1,), (1,)), ((), ())), preferred_element_type=f32)


def mm_tn(x, y):
    return lax.dot_general(x, y, (((0,), (0,)), ((), ())), preferred_element_type=f32)


def pack_kernel(
    n_a, n_b, n_c, cap, s_rows, t_rows, s_keys, t_keys, r_keys, s_cnt, t_cnt, r_cnt, out
):
    def halves(keys_ref, cnt_ref):
        keys = keys_ref[...]
        slots = keys.shape[1]
        groups = slots // cap
        spread = (iota((groups, slots), 1) // cap == iota((groups, slots), 0)).astype(bf16)
        cnt = jnp.broadcast_to(cnt_ref[...].astype(f32).astype(bf16), (8, groups))
        live = (iota((1, slots), 1) % cap).astype(f32) < mm(cnt, spread)[0:1]
        first = jnp.where(live, (keys // KEYS).astype(f32), -1.0)
        second = jnp.where(live, (keys % KEYS).astype(f32), -1.0)
        return first, second

    def at(vec, start):
        row = vec[:, start // LANES * LANES : (start // LANES + 1) * LANES]
        return pltpu.roll(row, (LANES - start % LANES) % LANES, 1) if start % LANES else row

    sb, sc = halves(s_keys, s_cnt)
    ta, tc = halves(t_keys, t_cnt)
    ra, rb = halves(r_keys, r_cnt)
    seg = n_c * cap
    row = iota((META, LANES), 0)
    for a in range(n_a):
        for b in range(n_b):
            rows = (
                at(sb, b * seg),
                at(sc, b * seg),
                at(ta, a * seg),
                at(tc, a * seg),
                at(ra, (a * n_b + b) * cap),
                at(rb, (a * n_b + b) * cap),
            )
            meta = jnp.zeros((META, LANES), f32)
            for k, value in enumerate(rows):
                meta = jnp.where(row == k, value, meta)
            meta = meta.astype(bf16)
            for c in range(n_c):
                d = (a * n_b + b) * n_c + c
                g, h = b * n_c + c, a * n_c + c
                out[d, 0:cap, :] = s_rows[g * cap : (g + 1) * cap, :]
                out[d, cap : 2 * cap, :] = t_rows[h * cap : (h + 1) * cap, :]
                out[d, 2 * cap : 2 * cap + META, :] = meta


def join_kernel(n_c, cap, srcs, held, out, sb_ref, sc_ref, ta_ref, tc_ref, pq_ref, f_ref):
    blocks = held.shape[0] // srcs
    m = srcs * cap
    wide = n_c * KEYS
    own = lax.axis_index("col")
    place = iota((cap, LANES), 1) % cap == iota((cap, LANES), 0)
    lane_c = iota((LANES, wide), 0) // cap
    sel_all = (lane_c == iota((LANES, wide), 1) // KEYS).astype(bf16)
    sel_first = (lane_c == 0).astype(bf16)
    here = iota((m, wide), 1) // KEYS == own
    key_all = (iota((m, wide), 1) % KEYS).astype(f32)

    def onehot(meta, kind, sel):
        rep = jnp.broadcast_to(meta[:, kind : kind + 1, :], (srcs, cap, LANES))
        rep = jnp.where(place[None], rep, 0.0).astype(bf16).reshape(m, LANES)
        return mm(rep, sel) == key_all

    def tables(i):
        meta = held[pl.ds(i * srcs, srcs), 2 * cap : 2 * cap + META, :].astype(f32)
        at = pl.ds(i * m, m)
        sb = onehot(meta, 0, sel_all)
        sc = onehot(meta, 1, sel_all)
        ta = onehot(meta, 2, sel_all)
        tc = onehot(meta, 3, sel_all)
        f_ref[0] += mm_tn(sb.astype(bf16), sc.astype(bf16))
        f_ref[1] += mm_tn(ta.astype(bf16), tc.astype(bf16))
        sb_ref[at] = (sb & here).astype(bf16)
        sc_ref[at] = (sc & here).astype(bf16)
        ta_ref[at] = (ta & here).astype(bf16)
        tc_ref[at] = (tc & here).astype(bf16)

    def joins(i):
        meta = held[pl.ds(i * srcs, srcs), 2 * cap : 2 * cap + META, :].astype(f32)
        ra = onehot(meta, 4, sel_first).astype(bf16)
        rb = onehot(meta, 5, sel_first).astype(bf16)
        xa = mm(ra, pq_ref[2]) + mm(ra, pq_ref[3])
        xb = mm(rb, pq_ref[0]) + mm(rb, pq_ref[1])
        triangles = jnp.sum(xa * xb, axis=1, keepdims=True)
        scale = 1.0 / jnp.sqrt(1.0 + triangles)
        xa_hi, xa_lo = split(xa)
        xb_hi, xb_lo = split(xb)

        def one(j, acc):
            at = pl.ds(j * m, m)
            sb, sc, ta, tc = sb_ref[at], sc_ref[at], ta_ref[at], tc_ref[at]
            rows = held[pl.ds(j * srcs, srcs), 0 : 2 * cap, :]
            s = rows[:, 0:cap, :].reshape(m, LANES)
            t = rows[:, cap : 2 * cap, :].reshape(m, LANES)
            hi, lo = split((mm_nt(xa_hi, sc) + mm_nt(xa_lo, sc)) * mm_nt(rb, sb))
            acc = acc + mm(hi, s) + mm(lo, s)
            hi, lo = split((mm_nt(xb_hi, tc) + mm_nt(xb_lo, tc)) * mm_nt(ra, ta))
            return acc + mm(hi, t) + mm(lo, t)

        acc = jnp.zeros((m, LANES), f32)
        acc = one(0, acc) if blocks == 1 else lax.fori_loop(0, blocks, one, acc)
        out[pl.ds(i * srcs, srcs)] = (acc * scale).reshape(srcs, cap, LANES)

    def each(step):
        if blocks == 1:
            step(0)
        else:
            pl.loop(0, blocks)(step)

    f_ref[...] = jnp.zeros_like(f_ref)
    each(tables)
    same = iota((wide, wide), 0) // KEYS == iota((wide, wide), 1) // KEYS
    for k in range(2):
        hi, lo = split(jnp.where(same, f_ref[k], 0.0))
        pq_ref[2 * k] = hi
        pq_ref[2 * k + 1] = lo
    each(joins)


def body(sizes, r_rows, r_keys, r_counts, s_rows, s_keys, s_counts, t_rows, t_keys, t_counts):
    n_a, n_b, n_c = sizes
    n = n_a * n_b * n_c
    cap = r_keys.shape[0] // r_counts.shape[0]
    width = r_rows.shape[1]
    srcs = max(512 // cap, 1)
    srcs = srcs if n % srcs == 0 else n
    total_slots = n * cap
    wide = n_c * KEYS
    row = lambda x: x.reshape(1, x.shape[0])
    packed = pl.pallas_call(
        functools.partial(pack_kernel, n_a, n_b, n_c, cap),
        out_shape=jax.ShapeDtypeStruct((n, 2 * cap + META, width), bf16),
        name="pack",
    )(
        s_rows, t_rows, row(s_keys), row(t_keys), row(r_keys),
        row(s_counts), row(t_counts), row(r_counts),
    )
    held = lax.all_to_all(packed, AXES, split_axis=0, concat_axis=0, tiled=True)
    shares = pl.pallas_call(
        functools.partial(join_kernel, n_c, cap, srcs),
        out_shape=jax.ShapeDtypeStruct((n, cap, width), f32),
        scratch_shapes=[pltpu.VMEM((total_slots, wide), bf16) for _ in range(4)]
        + [pltpu.VMEM((4, wide, wide), bf16), pltpu.VMEM((2, wide, wide), f32)],
        name="join",
    )(held)
    back = lax.all_to_all(shares, AXES, split_axis=0, concat_axis=0, tiled=True)
    total = jnp.sum(back.reshape(n_a * n_b, n_c, cap, width), axis=1)
    return (r_rows.astype(f32) * total.reshape(r_rows.shape)).astype(bf16)


def solution(mesh):
    rows, flat = P(AXES, None), P(AXES)
    sizes = tuple(mesh.shape[name] for name in AXES)
    return jax.shard_map(
        functools.partial(body, sizes),
        mesh=mesh,
        in_specs=(rows, flat, flat) * 3,
        out_specs=rows,
        check_vma=False,
    )
```

```python
import functools

import jax
import jax.numpy as jnp
from jax import lax
from jax.experimental import pallas as pl
from jax.experimental.pallas import tpu as pltpu
from jax.sharding import PartitionSpec as P

KEYS = 64
LANES = 128
META = 8
AXES = ("aa", "ba", "col")
f32 = jnp.float32
bf16 = jnp.bfloat16


def iota(shape, dim):
    return lax.broadcasted_iota(jnp.int32, shape, dim)


def split(x):
    hi = x.astype(bf16)
    return hi, (x - hi.astype(f32)).astype(bf16)


def mm(x, y):
    return lax.dot_general(x, y, (((1,), (0,)), ((), ())), preferred_element_type=f32)


def mm_nt(x, y):
    return lax.dot_general(x, y, (((1,), (1,)), ((), ())), preferred_element_type=f32)


def mm_tn(x, y):
    return lax.dot_general(x, y, (((0,), (0,)), ((), ())), preferred_element_type=f32)


def pack_kernel(
    n_a, n_b, n_c, cap, s_rows, t_rows, s_keys, t_keys, r_keys, s_cnt, t_cnt, r_cnt, r_rows, out, r_out
):
    def halves(keys_ref, cnt_ref):
        keys = keys_ref[...]
        slots = keys.shape[1]
        groups = slots // cap
        spread = (iota((groups, slots), 1) // cap == iota((groups, slots), 0)).astype(bf16)
        cnt = jnp.broadcast_to(cnt_ref[...].astype(f32).astype(bf16), (8, groups))
        live = (iota((1, slots), 1) % cap).astype(f32) < mm(cnt, spread)[0:1]
        first = jnp.where(live, (keys // KEYS).astype(f32), -1.0)
        second = jnp.where(live, (keys % KEYS).astype(f32), -1.0)
        return first, second

    def at(vec, start):
        row = vec[:, start // LANES * LANES : (start // LANES + 1) * LANES]
        return pltpu.roll(row, (LANES - start % LANES) % LANES, 1) if start % LANES else row

    r_out[...] = r_rows[...]
    sb, sc = halves(s_keys, s_cnt)
    ta, tc = halves(t_keys, t_cnt)
    ra, rb = halves(r_keys, r_cnt)
    seg = n_c * cap
    row = iota((META, LANES), 0)
    for a in range(n_a):
        for b in range(n_b):
            rows = (
                at(sb, b * seg),
                at(sc, b * seg),
                at(ta, a * seg),
                at(tc, a * seg),
                at(ra, (a * n_b + b) * cap),
                at(rb, (a * n_b + b) * cap),
            )
            meta = jnp.zeros((META, LANES), f32)
            for k, value in enumerate(rows):
                meta = jnp.where(row == k, value, meta)
            meta = meta.astype(bf16)
            for c in range(n_c):
                d = (a * n_b + b) * n_c + c
                g, h = b * n_c + c, a * n_c + c
                out[d, 0:cap, :] = s_rows[g * cap : (g + 1) * cap, :]
                out[d, cap : 2 * cap, :] = t_rows[h * cap : (h + 1) * cap, :]
                out[d, 2 * cap : 2 * cap + META, :] = meta


def home_kernel(shares, r_rows, out):
    groups, n_c, cap, width = shares.shape
    total = shares[:, 0]
    for c in range(1, n_c):
        total = total + shares[:, c]
    out[...] = (r_rows[...].astype(f32) * total.reshape(out.shape)).astype(bf16)


def join_kernel(n_c, cap, srcs, held, out, sb_ref, sc_ref, ta_ref, tc_ref, pq_ref, f_ref):
    blocks = held.shape[0] // srcs
    m = srcs * cap
    wide = n_c * KEYS
    own = lax.axis_index("col")
    place = iota((cap, LANES), 1) % cap == iota((cap, LANES), 0)
    lane_c = iota((LANES, wide), 0) // cap
    sel_all = (lane_c == iota((LANES, wide), 1) // KEYS).astype(bf16)
    sel_first = (lane_c == 0).astype(bf16)
    here = iota((m, wide), 1) // KEYS == own
    key_all = (iota((m, wide), 1) % KEYS).astype(f32)

    def onehot(meta, kind, sel):
        rep = jnp.broadcast_to(meta[:, kind : kind + 1, :], (srcs, cap, LANES))
        rep = jnp.where(place[None], rep, 0.0).astype(bf16).reshape(m, LANES)
        return mm(rep, sel) == key_all

    def tables(i):
        meta = held[pl.ds(i * srcs, srcs), 2 * cap : 2 * cap + META, :].astype(f32)
        at = pl.ds(i * m, m)
        sb = onehot(meta, 0, sel_all)
        sc = onehot(meta, 1, sel_all)
        ta = onehot(meta, 2, sel_all)
        tc = onehot(meta, 3, sel_all)
        f_ref[0] += mm_tn(sb.astype(bf16), sc.astype(bf16))
        f_ref[1] += mm_tn(ta.astype(bf16), tc.astype(bf16))
        sb_ref[at] = (sb & here).astype(bf16)
        sc_ref[at] = (sc & here).astype(bf16)
        ta_ref[at] = (ta & here).astype(bf16)
        tc_ref[at] = (tc & here).astype(bf16)

    def joins(i):
        meta = held[pl.ds(i * srcs, srcs), 2 * cap : 2 * cap + META, :].astype(f32)
        ra = onehot(meta, 4, sel_first).astype(bf16)
        rb = onehot(meta, 5, sel_first).astype(bf16)
        xa = mm(ra, pq_ref[2]) + mm(ra, pq_ref[3])
        xb = mm(rb, pq_ref[0]) + mm(rb, pq_ref[1])
        triangles = jnp.sum(xa * xb, axis=1, keepdims=True)
        scale = 1.0 / jnp.sqrt(1.0 + triangles)
        xa_hi, xa_lo = split(xa)
        xb_hi, xb_lo = split(xb)

        def one(j, acc):
            at = pl.ds(j * m, m)
            sb, sc, ta, tc = sb_ref[at], sc_ref[at], ta_ref[at], tc_ref[at]
            rows = held[pl.ds(j * srcs, srcs), 0 : 2 * cap, :]
            s = rows[:, 0:cap, :].reshape(m, LANES)
            t = rows[:, cap : 2 * cap, :].reshape(m, LANES)
            hi, lo = split((mm_nt(xa_hi, sc) + mm_nt(xa_lo, sc)) * mm_nt(rb, sb))
            acc = acc + mm(hi, s) + mm(lo, s)
            hi, lo = split((mm_nt(xb_hi, tc) + mm_nt(xb_lo, tc)) * mm_nt(ra, ta))
            return acc + mm(hi, t) + mm(lo, t)

        acc = jnp.zeros((m, LANES), f32)
        acc = one(0, acc) if blocks == 1 else lax.fori_loop(0, blocks, one, acc)
        out[pl.ds(i * srcs, srcs)] = (acc * scale).reshape(srcs, cap, LANES)

    def each(step):
        if blocks == 1:
            step(0)
        else:
            pl.loop(0, blocks)(step)

    f_ref[...] = jnp.zeros_like(f_ref)
    each(tables)
    same = iota((wide, wide), 0) // KEYS == iota((wide, wide), 1) // KEYS
    for k in range(2):
        hi, lo = split(jnp.where(same, f_ref[k], 0.0))
        pq_ref[2 * k] = hi
        pq_ref[2 * k + 1] = lo
    each(joins)


def body(sizes, r_rows, r_keys, r_counts, s_rows, s_keys, s_counts, t_rows, t_keys, t_counts):
    n_a, n_b, n_c = sizes
    n = n_a * n_b * n_c
    cap = r_keys.shape[0] // r_counts.shape[0]
    width = r_rows.shape[1]
    srcs = max(512 // cap, 1)
    srcs = srcs if n % srcs == 0 else n
    total_slots = n * cap
    wide = n_c * KEYS
    row = lambda x: x.reshape(1, x.shape[0])
    near = lambda x: pltpu.with_memory_space_constraint(x, pltpu.VMEM)
    params = pltpu.CompilerParams(vmem_limit_bytes=40 << 20)
    packed, r_kept = pl.pallas_call(
        functools.partial(pack_kernel, n_a, n_b, n_c, cap),
        out_shape=(pltpu.VMEM((n, 2 * cap + META, width), bf16), pltpu.VMEM(r_rows.shape, bf16)),
        compiler_params=params,
        name="pack",
    )(
        s_rows, t_rows, row(s_keys), row(t_keys), row(r_keys),
        row(s_counts), row(t_counts), row(r_counts), r_rows,
    )
    held = lax.all_to_all(packed, AXES, split_axis=0, concat_axis=0, tiled=True)
    shares = pl.pallas_call(
        functools.partial(join_kernel, n_c, cap, srcs),
        out_shape=pltpu.VMEM((n, cap, width), f32),
        scratch_shapes=[pltpu.VMEM((total_slots, wide), bf16) for _ in range(4)]
        + [pltpu.VMEM((4, wide, wide), bf16), pltpu.VMEM((2, wide, wide), f32)],
        compiler_params=params,
        name="join",
    )(near(held))
    back = lax.all_to_all(shares, AXES, split_axis=0, concat_axis=0, tiled=True)
    return pl.pallas_call(
        home_kernel,
        out_shape=jax.ShapeDtypeStruct(r_rows.shape, bf16),
        compiler_params=params,
        name="home",
    )(near(back.reshape(n_a * n_b, n_c, cap, width)), near(r_kept))


def solution(mesh):
    rows, flat = P(AXES, None), P(AXES)
    sizes = tuple(mesh.shape[name] for name in AXES)
    return jax.shard_map(
        functools.partial(body, sizes),
        mesh=mesh,
        in_specs=(rows, flat, flat) * 3,
        out_specs=rows,
        check_vma=False,
    )
```

```python
import functools

import jax
import jax.numpy as jnp
from jax import lax
from jax.experimental import pallas as pl
from jax.experimental.pallas import tpu as pltpu
from jax.sharding import PartitionSpec as P

KEYS = 64
LANES = 128
META = 8
AXES = ("aa", "ba", "col")
f32 = jnp.float32
bf16 = jnp.bfloat16


def iota(shape, dim):
    return lax.broadcasted_iota(jnp.int32, shape, dim)


def split(x):
    hi = x.astype(bf16)
    return hi, (x - hi.astype(f32)).astype(bf16)


def mm(x, y):
    return lax.dot_general(x, y, (((1,), (0,)), ((), ())), preferred_element_type=f32)


def mm_nt(x, y):
    return lax.dot_general(x, y, (((1,), (1,)), ((), ())), preferred_element_type=f32)


def mm_tn(x, y):
    return lax.dot_general(x, y, (((0,), (0,)), ((), ())), preferred_element_type=f32)


def pack_kernel(
    n_a, n_b, n_c, cap,
    s_rows, t_rows, r_rows, s_keys, t_keys, r_keys, s_cnt, t_cnt, r_cnt,
    out, r_out,
    s_keys_near, t_keys_near, r_keys_near, s_cnt_near, t_cnt_near, r_cnt_near, sem_small, sem_rows,
):
    small = [
        pltpu.make_async_copy(far, near, sem_small.at[i])
        for i, (far, near) in enumerate(
            (
                (s_keys, s_keys_near),
                (t_keys, t_keys_near),
                (r_keys, r_keys_near),
                (s_cnt, s_cnt_near),
                (t_cnt, t_cnt_near),
                (r_cnt, r_cnt_near),
            )
        )
    ]
    rows = []

    def send(far, near):
        rows.append(pltpu.make_async_copy(far, near, sem_rows.at[len(rows)]))

    for a in range(n_a):
        send(s_rows, out.at[pl.ds(a * n_b * n_c, n_b * n_c), pl.ds(0, cap), :])
        for b in range(n_b):
            d = (a * n_b + b) * n_c
            send(t_rows.at[pl.ds(a * n_c, n_c)], out.at[pl.ds(d, n_c), pl.ds(cap, cap), :])
    send(r_rows, r_out)
    for copy in small + rows:
        copy.start()

    def halves(keys_ref, cnt_ref):
        keys = keys_ref[...]
        slots = keys.shape[1]
        groups = slots // cap
        spread = (iota((groups, slots), 1) // cap == iota((groups, slots), 0)).astype(bf16)
        cnt = jnp.broadcast_to(cnt_ref[...].astype(f32).astype(bf16), (8, groups))
        live = (iota((1, slots), 1) % cap).astype(f32) < mm(cnt, spread)[0:1]
        first = jnp.where(live, lax.div(keys, KEYS).astype(f32), -1.0)
        second = jnp.where(live, lax.rem(keys, KEYS).astype(f32), -1.0)
        return first, second

    def at(vec, start):
        row = vec[:, start // LANES * LANES : (start // LANES + 1) * LANES]
        return pltpu.roll(row, (LANES - start % LANES) % LANES, 1) if start % LANES else row

    for copy in small:
        copy.wait()
    sb, sc = halves(s_keys_near, s_cnt_near)
    ta, tc = halves(t_keys_near, t_cnt_near)
    ra, rb = halves(r_keys_near, r_cnt_near)
    seg = n_c * cap
    row = iota((META, LANES), 0)
    for a in range(n_a):
        for b in range(n_b):
            vecs = (
                at(sb, b * seg),
                at(sc, b * seg),
                at(ta, a * seg),
                at(tc, a * seg),
                at(ra, (a * n_b + b) * cap),
                at(rb, (a * n_b + b) * cap),
            )
            meta = jnp.zeros((META, LANES), f32)
            for k, value in enumerate(vecs):
                meta = jnp.where(row == k, value, meta)
            meta = meta.astype(bf16)
            for c in range(n_c):
                out[(a * n_b + b) * n_c + c, 2 * cap : 2 * cap + META, :] = meta
    for copy in rows:
        copy.wait()


def home_kernel(shares, r_rows, out):
    groups, n_c, cap, width = shares.shape
    total = shares[:, 0]
    for c in range(1, n_c):
        total = total + shares[:, c]
    out[...] = (r_rows[...].astype(f32) * total.reshape(out.shape)).astype(bf16)


def join_kernel(n_c, cap, srcs, held, out, sb_ref, sc_ref, ta_ref, tc_ref, pq_ref, f_ref):
    blocks = held.shape[0] // srcs
    m = srcs * cap
    wide = n_c * KEYS
    own = lax.axis_index("col")
    place = iota((cap, LANES), 1) % cap == iota((cap, LANES), 0)
    lane_c = iota((LANES, wide), 0) // cap
    sel_all = (lane_c == iota((LANES, wide), 1) // KEYS).astype(bf16)
    sel_first = (lane_c == 0).astype(bf16)
    here = iota((m, wide), 1) // KEYS == own
    key_all = (iota((m, wide), 1) % KEYS).astype(f32)

    def onehot(meta, kind, sel):
        rep = jnp.broadcast_to(meta[:, kind : kind + 1, :], (srcs, cap, LANES))
        rep = jnp.where(place[None], rep, 0.0).astype(bf16).reshape(m, LANES)
        return mm(rep, sel) == key_all

    def tables(i):
        meta = held[pl.ds(i * srcs, srcs), 2 * cap : 2 * cap + META, :].astype(f32)
        at = pl.ds(i * m, m)
        sb = onehot(meta, 0, sel_all)
        sc = onehot(meta, 1, sel_all)
        ta = onehot(meta, 2, sel_all)
        tc = onehot(meta, 3, sel_all)
        f_ref[0] += mm_tn(sb.astype(bf16), sc.astype(bf16))
        f_ref[1] += mm_tn(ta.astype(bf16), tc.astype(bf16))
        sb_ref[at] = (sb & here).astype(bf16)
        sc_ref[at] = (sc & here).astype(bf16)
        ta_ref[at] = (ta & here).astype(bf16)
        tc_ref[at] = (tc & here).astype(bf16)

    def joins(i):
        meta = held[pl.ds(i * srcs, srcs), 2 * cap : 2 * cap + META, :].astype(f32)
        ra = onehot(meta, 4, sel_first).astype(bf16)
        rb = onehot(meta, 5, sel_first).astype(bf16)
        xa = mm(ra, pq_ref[2]) + mm(ra, pq_ref[3])
        xb = mm(rb, pq_ref[0]) + mm(rb, pq_ref[1])
        triangles = jnp.sum(xa * xb, axis=1, keepdims=True)
        scale = 1.0 / jnp.sqrt(1.0 + triangles)
        xa_hi, xa_lo = split(xa)
        xb_hi, xb_lo = split(xb)

        def one(j, acc):
            at = pl.ds(j * m, m)
            sb, sc, ta, tc = sb_ref[at], sc_ref[at], ta_ref[at], tc_ref[at]
            rows = held[pl.ds(j * srcs, srcs), 0 : 2 * cap, :]
            s = rows[:, 0:cap, :].reshape(m, LANES)
            t = rows[:, cap : 2 * cap, :].reshape(m, LANES)
            hi, lo = split((mm_nt(xa_hi, sc) + mm_nt(xa_lo, sc)) * mm_nt(rb, sb))
            acc = acc + mm(hi, s) + mm(lo, s)
            hi, lo = split((mm_nt(xb_hi, tc) + mm_nt(xb_lo, tc)) * mm_nt(ra, ta))
            return acc + mm(hi, t) + mm(lo, t)

        acc = jnp.zeros((m, LANES), f32)
        acc = one(0, acc) if blocks == 1 else lax.fori_loop(0, blocks, one, acc)
        out[pl.ds(i * srcs, srcs)] = (acc * scale).reshape(srcs, cap, LANES)

    def each(step):
        if blocks == 1:
            step(0)
        else:
            pl.loop(0, blocks)(step)

    f_ref[...] = jnp.zeros_like(f_ref)
    each(tables)
    same = iota((wide, wide), 0) // KEYS == iota((wide, wide), 1) // KEYS
    for k in range(2):
        hi, lo = split(jnp.where(same, f_ref[k], 0.0))
        pq_ref[2 * k] = hi
        pq_ref[2 * k + 1] = lo
    each(joins)


def body(sizes, r_rows, r_keys, r_counts, s_rows, s_keys, s_counts, t_rows, t_keys, t_counts):
    n_a, n_b, n_c = sizes
    n = n_a * n_b * n_c
    cap = r_keys.shape[0] // r_counts.shape[0]
    width = r_rows.shape[1]
    srcs = max(512 // cap, 1)
    srcs = srcs if n % srcs == 0 else n
    total_slots = n * cap
    wide = n_c * KEYS
    row = lambda x: x.reshape(1, x.shape[0])
    far = lambda x: pltpu.with_memory_space_constraint(x, pltpu.HBM)
    near = lambda x: pltpu.with_memory_space_constraint(x, pltpu.VMEM)
    params = pltpu.CompilerParams(vmem_limit_bytes=40 << 20)
    small = (row(s_keys), row(t_keys), row(r_keys), row(s_counts), row(t_counts), row(r_counts))
    packed, r_kept = pl.pallas_call(
        functools.partial(pack_kernel, n_a, n_b, n_c, cap),
        in_specs=[pl.BlockSpec(memory_space=pltpu.HBM)] * 9,
        out_shape=(pltpu.VMEM((n, 2 * cap + META, width), bf16), pltpu.VMEM(r_rows.shape, bf16)),
        scratch_shapes=[pltpu.VMEM(x.shape, x.dtype) for x in small]
        + [
            pltpu.SemaphoreType.DMA((len(small),)),
            pltpu.SemaphoreType.DMA((n_a + n_a * n_b + 1,)),
        ],
        compiler_params=params,
        name="pack",
    )(
        *map(
            far,
            (s_rows.reshape(n_b * n_c, cap, width), t_rows.reshape(n_a * n_c, cap, width), r_rows)
            + small,
        )
    )
    held = lax.all_to_all(packed, AXES, split_axis=0, concat_axis=0, tiled=True)
    shares = pl.pallas_call(
        functools.partial(join_kernel, n_c, cap, srcs),
        out_shape=pltpu.VMEM((n, cap, width), f32),
        scratch_shapes=[pltpu.VMEM((total_slots, wide), bf16) for _ in range(4)]
        + [pltpu.VMEM((4, wide, wide), bf16), pltpu.VMEM((2, wide, wide), f32)],
        compiler_params=params,
        name="join",
    )(near(held))
    back = lax.all_to_all(shares, AXES, split_axis=0, concat_axis=0, tiled=True)
    return pl.pallas_call(
        home_kernel,
        out_shape=jax.ShapeDtypeStruct(r_rows.shape, bf16),
        compiler_params=params,
        name="home",
    )(near(back.reshape(n_a * n_b, n_c, cap, width)), near(r_kept))


def solution(mesh):
    rows, flat = P(AXES, None), P(AXES)
    sizes = tuple(mesh.shape[name] for name in AXES)
    return jax.shard_map(
        functools.partial(body, sizes),
        mesh=mesh,
        in_specs=(rows, flat, flat) * 3,
        out_specs=rows,
        check_vma=False,
    )
```

```python
import functools

import jax
import jax.numpy as jnp
from jax import lax
from jax.experimental import pallas as pl
from jax.experimental.pallas import tpu as pltpu
from jax.sharding import PartitionSpec as P

KEYS = 64
LANES = 128
META = 8
AXES = ("aa", "ba", "col")
f32 = jnp.float32
bf16 = jnp.bfloat16


def iota(shape, dim):
    return lax.broadcasted_iota(jnp.int32, shape, dim)


def split(x):
    hi = x.astype(bf16)
    return hi, (x - hi.astype(f32)).astype(bf16)


def mm(x, y):
    return lax.dot_general(x, y, (((1,), (0,)), ((), ())), preferred_element_type=f32)


def mm_nt(x, y):
    return lax.dot_general(x, y, (((1,), (1,)), ((), ())), preferred_element_type=f32)


def mm_tn(x, y):
    return lax.dot_general(x, y, (((0,), (0,)), ((), ())), preferred_element_type=f32)


def swap(x, y):
    half = x.shape[-1] // 2
    low = iota(x.shape, x.ndim - 1) < half
    turn = lambda v: pltpu.roll(v, half, v.ndim - 1)
    return jnp.where(low, x, turn(y)), jnp.where(low, turn(x), y)


def pack_kernel(
    n_a, n_b, n_c, cap, split_w,
    s_rows, t_rows, r_rows, s_keys, t_keys, r_keys, s_cnt, t_cnt, r_cnt,
    out, r_out,
    s_near, t_near,
    s_keys_near, t_keys_near, r_keys_near, s_cnt_near, t_cnt_near, r_cnt_near, sem,
):
    small = [
        pltpu.make_async_copy(far, near, sem.at[i])
        for i, (far, near) in enumerate(
            (
                (s_keys, s_keys_near),
                (t_keys, t_keys_near),
                (r_keys, r_keys_near),
                (s_cnt, s_cnt_near),
                (t_cnt, t_cnt_near),
                (r_cnt, r_cnt_near),
            )
        )
    ]
    rows = [
        pltpu.make_async_copy(far, near, sem.at[len(small) + i])
        for i, (far, near) in enumerate(((s_rows, s_near), (t_rows, t_near), (r_rows, r_out)))
    ]
    for copy in small + rows:
        copy.start()

    def halves(keys_ref, cnt_ref):
        keys = keys_ref[...]
        slots = keys.shape[1]
        groups = slots // cap
        spread = (iota((groups, slots), 1) // cap == iota((groups, slots), 0)).astype(bf16)
        cnt = jnp.broadcast_to(cnt_ref[...].astype(f32).astype(bf16), (8, groups))
        live = (iota((1, slots), 1) % cap).astype(f32) < mm(cnt, spread)[0:1]
        first = jnp.where(live, lax.div(keys, KEYS).astype(f32), -1.0)
        second = jnp.where(live, lax.rem(keys, KEYS).astype(f32), -1.0)
        return first, second

    def at(vec, start):
        row = vec[:, start // LANES * LANES : (start // LANES + 1) * LANES]
        return pltpu.roll(row, (LANES - start % LANES) % LANES, 1) if start % LANES else row

    for copy in small:
        copy.wait()
    sb, sc = halves(s_keys_near, s_cnt_near)
    ta, tc = halves(t_keys_near, t_cnt_near)
    ra, rb = halves(r_keys_near, r_cnt_near)
    seg = n_c * cap
    row = iota((META, LANES), 0)

    def ring(vec, start):
        out = at(vec, start)
        size = seg
        while size < LANES:
            out = jnp.where(iota((1, LANES), 1) < size, out, pltpu.roll(out, size, 1))
            size *= 2
        return out

    s_meta = [(ring(sb, b * seg), ring(sc, b * seg)) for b in range(n_b)]
    t_meta = [(ring(ta, a * seg), ring(tc, a * seg)) for a in range(n_a)]
    for a in range(n_a):
        for b in range(n_b):
            meta = jnp.zeros((META, LANES), f32)
            for k, value in enumerate(s_meta[b] + t_meta[a]):
                meta = jnp.where(row == k, value, meta)
            r_at = (a * n_b + b) * cap
            for c in range(0, n_c, split_w):
                turned = pltpu.roll(meta, LANES - c * cap, 1) if c else meta
                for k, vec in ((4, ra), (5, rb)):
                    turned = jnp.where(row == k, at(vec, r_at), turned)
                turned = turned.astype(bf16)
                for w in range(split_w):
                    out[(a * n_b + b) * n_c + c + w, 2 * cap : 2 * cap + META, :] = turned
    for copy in rows:
        copy.wait()

    def parts(near, g):
        if split_w == 1:
            return (near[g],)
        pair = swap(near[g].astype(f32), near[g + 1].astype(f32))
        return tuple(x.astype(bf16) for x in pair)

    for c in range(0, n_c, split_w):
        for b in range(n_b):
            for w, part in enumerate(parts(s_near, b * n_c + c)):
                for a in range(n_a):
                    out[(a * n_b + b) * n_c + c + w, 0:cap, :] = part
        for a in range(n_a):
            for w, part in enumerate(parts(t_near, a * n_c + c)):
                for b in range(n_b):
                    out[(a * n_b + b) * n_c + c + w, cap : 2 * cap, :] = part


def home_kernel(split_w, shares, r_rows, out):
    groups, n_c, cap_w, width = shares.shape
    total = [shares[:, w] for w in range(split_w)]
    for c in range(split_w, n_c):
        total[c % split_w] = total[c % split_w] + shares[:, c]
    if split_w == 2:
        total = swap(*total)
    for w in range(split_w):
        at = pl.ds(w * cap_w, cap_w)
        out[:, at, :] = (r_rows[:, at, :].astype(f32) * total[w]).astype(bf16)


BIG = 2.0**15


def join_kernel(n_c, cap, split_w, srcs, held, out, sb_ref, sc_ref, ta_ref, tc_ref, f_ref):
    blocks = held.shape[0] // srcs
    m = srcs * cap
    key_in = lambda shape, dim: (iota(shape, dim) % KEYS).astype(f32)
    place = iota((cap, LANES), 1) % cap == iota((cap, LANES), 0)
    order_c = [i for i in range(split_w) for _ in range(2)] + list(range(split_w, n_c))
    order_c += [-2] * (len(order_c) % 2)
    order_b = list(range(n_c)) + [-1] * (n_c % 2)
    wide_b, wide_c = len(order_b) * KEYS, len(order_c) * KEYS

    def bucket(order, shape, dim):
        block = iota(shape, dim) // KEYS
        at = jnp.full(shape, order[0], jnp.int32)
        for k in range(1, len(order)):
            at = jnp.where(block == k, order[k], at)
        return at

    lane_b = iota((LANES, wide_b), 0) // cap
    lane_c = iota((LANES, wide_c), 0) // cap
    sel_b = (lane_b == bucket(order_b, (LANES, wide_b), 1)).astype(bf16)
    sel_c = (lane_c == bucket(order_c, (LANES, wide_c), 1)).astype(bf16)
    sel_r = (iota((LANES, LANES), 0) < cap).astype(bf16)

    def onehot(meta, kind, sel):
        rep = jnp.broadcast_to(meta[:, kind : kind + 1, :], (srcs, cap, LANES))
        rep = jnp.where(place[None], rep, 0.0).astype(bf16).reshape(m, LANES)
        return mm(rep, sel) == key_in((m, sel.shape[1]), 1)

    def meta_of(i):
        return held[pl.ds(i * srcs, srcs), 2 * cap : 2 * cap + META, :].astype(f32)

    own_b, own_c = LANES, split_w * LANES

    def tables(i):
        meta = meta_of(i)
        at = pl.ds(i * m, m)
        for k, (b_ref, c_ref) in enumerate(((sb_ref, sc_ref), (ta_ref, tc_ref))):
            b = onehot(meta, 2 * k, sel_b).astype(bf16)
            c = onehot(meta, 2 * k + 1, sel_c).astype(bf16)
            f_ref[k] += mm_tn(b, c)
            b_ref[at] = b[:, 0:own_b]
            c_ref[at] = c[:, 0:own_c]

    def counts(k):
        total = jnp.zeros((KEYS, wide_c), f32)
        at = bucket(order_c, (KEYS, wide_c), 1)
        for j, b in enumerate(order_b):
            total = total + jnp.where(at == b, f_ref[k, pl.ds(j * KEYS, KEYS), :], 0.0)
        return total

    def joins(gather_a, gather_b, i):
        meta = meta_of(i)
        ra = onehot(meta, 4, sel_r)
        rb = onehot(meta, 5, sel_r)
        va = mm(ra.astype(bf16), gather_a)
        vb = mm(rb.astype(bf16), gather_b)
        pick = [
            jnp.where(rb, va[:, k * LANES : (k + 1) * LANES], 0.0).astype(bf16)
            for k in range(split_w, split_w + 2)
        ]
        scale = mm(jnp.concatenate(pick, 1), jnp.ones((2 * LANES, LANES), bf16))
        low = iota((m, LANES), 1) < KEYS

        def sides(value, hot):
            flag = jnp.where(hot, BIG, 0.0)
            return [
                jnp.concatenate(
                    [
                        value[:, w * LANES : (w + 1) * LANES].astype(bf16),
                        jnp.where(low == (w == 0), flag, 0.0).astype(bf16),
                    ],
                    1,
                )
                for w in range(split_w)
            ]

        of_s, of_t = sides(va, rb), sides(vb, ra)

        def one(j, accs):
            at = pl.ds(j * m, m)
            rows = held[pl.ds(j * srcs, srcs), 0 : 2 * cap, :]
            accs = list(accs)
            for left, b_ref, c_ref, start in ((of_s, sb_ref, sc_ref, 0), (of_t, ta_ref, tc_ref, cap)):
                x = rows[:, start : start + cap, :].reshape(m, LANES)
                b = b_ref[at]
                for w in range(split_w):
                    right = jnp.concatenate([c_ref[at, w * LANES : (w + 1) * LANES], b], 1)
                    hi, lo = split(jnp.maximum(mm_nt(left[w], right) - BIG, 0.0))
                    accs[w] = accs[w] + mm(hi, x) + mm(lo, x)
            return tuple(accs)

        accs = tuple(jnp.zeros((m, LANES), f32) for _ in range(split_w))
        accs = one(0, accs) if blocks == 1 else lax.fori_loop(0, blocks, one, accs)
        accs = [(acc * scale).reshape(srcs, cap, LANES) for acc in accs]
        at = pl.ds(i * srcs, srcs)
        if split_w == 1:
            out[at] = accs[0]
        else:
            half = cap // 2
            turn = lambda v: pltpu.roll(v, LANES // 2, 2)
            first = accs[0][:, :half] + turn(accs[1][:, :half])
            second = turn(accs[0][:, half:]) + accs[1][:, half:]
            out[at] = jnp.where(iota((srcs, half, LANES), 2) < LANES // 2, first, second)

    def each(step):
        if blocks == 1:
            step(0)
        else:
            pl.loop(0, blocks)(step)

    f_ref[...] = jnp.zeros_like(f_ref)
    each(tables)
    s_counts, t_counts = counts(0), counts(1)
    once = (iota((KEYS, wide_c), 1) // KEYS % 2 == 0) | (iota((KEYS, wide_c), 1) >= own_c)
    s_parts, t_parts = split(s_counts), split(jnp.where(once, t_counts, 0.0))
    triangles = sum(mm_nt(t, s) for t in t_parts for s in s_parts)
    scale = 1.0 / jnp.sqrt(1.0 + triangles)
    hi, rest = split(scale)
    middle, rest = split(scale - hi.astype(f32))
    left = lambda x: iota(x.shape, 1) < KEYS

    def gather(count, tail):
        hi, lo = split(count[:, 0:own_c])
        first = iota(hi.shape, 1) % LANES < KEYS
        table = jnp.concatenate([jnp.where(first, hi.astype(f32), lo.astype(f32)), *tail], 1)
        table = table.astype(bf16)
        return jnp.concatenate([table, jnp.zeros_like(table)], 0)

    parts = [x.astype(f32) for x in (hi, middle, rest)] + [jnp.zeros((KEYS, KEYS), f32)]
    each(functools.partial(joins, gather(t_counts, parts), gather(s_counts, [])))


def body(sizes, r_rows, r_keys, r_counts, s_rows, s_keys, s_counts, t_rows, t_keys, t_counts):
    n_a, n_b, n_c = sizes
    n = n_a * n_b * n_c
    cap = r_keys.shape[0] // r_counts.shape[0]
    width = r_rows.shape[1]
    srcs = max(512 // cap, 1)
    srcs = srcs if n % srcs == 0 else n
    total_slots = n * cap
    split_w = 2 if n_c % 2 == 0 and width == LANES and cap % 16 == 0 else 1
    wide_b, wide_c = -(-n_c // 2) * LANES, -(-(n_c + split_w) // 2) * LANES
    row = lambda x: x.reshape(1, x.shape[0])
    far = lambda x: pltpu.with_memory_space_constraint(x, pltpu.HBM)
    near = lambda x: pltpu.with_memory_space_constraint(x, pltpu.VMEM)
    params = pltpu.CompilerParams(vmem_limit_bytes=40 << 20)
    small = (row(s_keys), row(t_keys), row(r_keys), row(s_counts), row(t_counts), row(r_counts))
    groups = (s_rows.shape[0] // cap, t_rows.shape[0] // cap, r_rows.shape[0] // cap)
    blocked = [x.reshape(g, cap, width) for x, g in zip((s_rows, t_rows, r_rows), groups)]
    near_like = lambda x: pltpu.VMEM(x.shape, x.dtype)
    packed, r_kept = pl.pallas_call(
        functools.partial(pack_kernel, n_a, n_b, n_c, cap, split_w),
        in_specs=[pl.BlockSpec(memory_space=pltpu.HBM)] * 9,
        out_shape=(pltpu.VMEM((n, 2 * cap + META, width), bf16), near_like(blocked[2])),
        scratch_shapes=[near_like(x) for x in (*blocked[:2], *small)]
        + [pltpu.SemaphoreType.DMA((9,))],
        compiler_params=params,
        name="pack",
    )(*map(far, (*blocked, *small)))
    held = lax.all_to_all(packed, AXES, split_axis=0, concat_axis=0, tiled=True)
    shares = pl.pallas_call(
        functools.partial(join_kernel, n_c, cap, split_w, srcs),
        out_shape=pltpu.VMEM((n, cap // split_w, width), f32),
        scratch_shapes=[
            pltpu.VMEM((total_slots, LANES), bf16),
            pltpu.VMEM((total_slots, split_w * LANES), bf16),
        ]
        * 2
        + [pltpu.VMEM((2, wide_b, wide_c), f32)],
        compiler_params=params,
        name="join",
    )(near(held))
    back = lax.all_to_all(shares, AXES, split_axis=0, concat_axis=0, tiled=True)
    joined = pl.pallas_call(
        functools.partial(home_kernel, split_w),
        out_shape=jax.ShapeDtypeStruct(blocked[2].shape, bf16),
        compiler_params=params,
        name="home",
    )(near(back.reshape(n_a * n_b, n_c, cap // split_w, width)), near(r_kept))
    return joined.reshape(r_rows.shape)


def solution(mesh):
    rows, flat = P(AXES, None), P(AXES)
    sizes = tuple(mesh.shape[name] for name in AXES)
    return jax.shard_map(
        functools.partial(body, sizes),
        mesh=mesh,
        in_specs=(rows, flat, flat) * 3,
        out_specs=rows,
        check_vma=False,
    )
```

```python
import functools

import jax
import jax.numpy as jnp
from jax import lax
from jax.experimental import pallas as pl
from jax.experimental.pallas import tpu as pltpu
from jax.sharding import PartitionSpec as P

KEYS = 64
LANES = 128
META = 8
AXES = ("aa", "ba", "col")
f32 = jnp.float32
bf16 = jnp.bfloat16


def iota(shape, dim):
    return lax.broadcasted_iota(jnp.int32, shape, dim)


def split(x):
    hi = x.astype(bf16)
    return hi, (x - hi.astype(f32)).astype(bf16)


def mm(x, y):
    return lax.dot_general(x, y, (((1,), (0,)), ((), ())), preferred_element_type=f32)


def mm_nt(x, y):
    return lax.dot_general(x, y, (((1,), (1,)), ((), ())), preferred_element_type=f32)


def mm_tn(x, y):
    return lax.dot_general(x, y, (((0,), (0,)), ((), ())), preferred_element_type=f32)


def swap(x, y):
    half = x.shape[-1] // 2
    low = iota(x.shape, x.ndim - 1) < half
    turn = lambda v: pltpu.roll(v, half, v.ndim - 1)
    return jnp.where(low, x, turn(y)), jnp.where(low, turn(x), y)


def pack_kernel(
    n_a, n_b, n_c, cap, split_w,
    s_rows, t_rows, r_rows, s_keys, t_keys, r_keys, s_cnt, t_cnt, r_cnt,
    out, r_out,
    s_near, t_near,
    s_keys_near, t_keys_near, r_keys_near, s_cnt_near, t_cnt_near, r_cnt_near, sem,
):
    small = [
        pltpu.make_async_copy(far, near, sem.at[i])
        for i, (far, near) in enumerate(
            (
                (s_keys, s_keys_near),
                (t_keys, t_keys_near),
                (r_keys, r_keys_near),
                (s_cnt, s_cnt_near),
                (t_cnt, t_cnt_near),
                (r_cnt, r_cnt_near),
            )
        )
    ]
    rows = [
        pltpu.make_async_copy(far, near, sem.at[len(small) + i])
        for i, (far, near) in enumerate(((s_rows, s_near), (t_rows, t_near), (r_rows, r_out)))
    ]
    for copy in small + rows:
        copy.start()

    def halves(keys_ref, cnt_ref):
        keys = keys_ref[...]
        slots = keys.shape[1]
        groups = slots // cap
        spread = (iota((groups, slots), 1) // cap == iota((groups, slots), 0)).astype(bf16)
        cnt = jnp.broadcast_to(cnt_ref[...].astype(f32).astype(bf16), (8, groups))
        live = (iota((1, slots), 1) % cap).astype(f32) < mm(cnt, spread)[0:1]
        first = jnp.where(live, lax.div(keys, KEYS).astype(f32), -1.0)
        second = jnp.where(live, lax.rem(keys, KEYS).astype(f32), -1.0)
        return first, second

    def at(vec, start):
        row = vec[:, start // LANES * LANES : (start // LANES + 1) * LANES]
        return pltpu.roll(row, (LANES - start % LANES) % LANES, 1) if start % LANES else row

    for copy in small:
        copy.wait()
    sb, sc = halves(s_keys_near, s_cnt_near)
    ta, tc = halves(t_keys_near, t_cnt_near)
    ra, rb = halves(r_keys_near, r_cnt_near)
    seg = n_c * cap
    row = iota((META, LANES), 0)

    def ring(vec, start):
        out = at(vec, start)
        size = seg
        while size < LANES:
            out = jnp.where(iota((1, LANES), 1) < size, out, pltpu.roll(out, size, 1))
            size *= 2
        return out

    s_meta = [(ring(sb, b * seg), ring(sc, b * seg)) for b in range(n_b)]
    t_meta = [(ring(ta, a * seg), ring(tc, a * seg)) for a in range(n_a)]
    for a in range(n_a):
        for b in range(n_b):
            meta = jnp.zeros((META, LANES), f32)
            for k, value in enumerate(s_meta[b] + t_meta[a]):
                meta = jnp.where(row == k, value, meta)
            r_at = (a * n_b + b) * cap
            for c in range(0, n_c, split_w):
                turned = pltpu.roll(meta, LANES - c * cap, 1) if c else meta
                for k, vec in ((4, ra), (5, rb)):
                    turned = jnp.where(row == k, at(vec, r_at), turned)
                turned = turned.astype(bf16)
                for w in range(split_w):
                    out[(a * n_b + b) * n_c + c + w, 2 * cap : 2 * cap + META, :] = turned
    for copy in rows:
        copy.wait()

    def parts(near, g):
        if split_w == 1:
            return (near[g],)
        pair = swap(near[g].astype(f32), near[g + 1].astype(f32))
        return tuple(x.astype(bf16) for x in pair)

    for c in range(0, n_c, split_w):
        for b in range(n_b):
            for w, part in enumerate(parts(s_near, b * n_c + c)):
                for a in range(n_a):
                    out[(a * n_b + b) * n_c + c + w, 0:cap, :] = part
        for a in range(n_a):
            for w, part in enumerate(parts(t_near, a * n_c + c)):
                for b in range(n_b):
                    out[(a * n_b + b) * n_c + c + w, cap : 2 * cap, :] = part


def home_kernel(split_w, shares, r_rows, out):
    groups, n_c, cap_w, width = shares.shape
    total = [shares[:, w] for w in range(split_w)]
    for c in range(split_w, n_c):
        total[c % split_w] = total[c % split_w] + shares[:, c]
    if split_w == 2:
        total = swap(*total)
    for w in range(split_w):
        at = pl.ds(w * cap_w, cap_w)
        out[:, at, :] = (r_rows[:, at, :].astype(f32) * total[w]).astype(bf16)


BIG = 2.0**15
EXACT = 256.0


def join_kernel(n_c, cap, split_w, srcs, held, out, s_ref, t_ref, f_ref):
    blocks = held.shape[0] // srcs
    m = srcs * cap
    wide = f_ref.shape[1]
    rows_of = LANES // split_w
    part = cap // split_w
    key_in = lambda shape, dim: (iota(shape, dim) % KEYS).astype(f32)
    place = iota((cap, LANES), 1) % cap == iota((cap, LANES), 0)
    sel = (iota((LANES, wide), 0) // cap == iota((LANES, wide), 1) // KEYS).astype(bf16)

    def meta_of(i):
        return held[pl.ds(i * srcs, srcs), 2 * cap : 2 * cap + META, :].astype(f32)

    def tables(i):
        meta = meta_of(i)

        def hot(kind):
            rep = jnp.broadcast_to(meta[:, kind : kind + 1, :], (srcs, cap, LANES))
            rep = jnp.where(place[None], rep, 0.0).astype(bf16).reshape(m, LANES)
            return (mm(rep, sel) == key_in((m, wide), 1)).astype(bf16)

        at = pl.ds(i * m, m)
        for k, ref in enumerate((s_ref, t_ref)):
            first, c = hot(2 * k), hot(2 * k + 1)
            if blocks == 1:
                f_ref[k] = mm_tn(first, c)
            else:
                f_ref[k] += mm_tn(first, c)
            ref[at, 0:LANES] = c[:, 0:LANES]
            ref[at, LANES : 2 * LANES] = first[:, 0:LANES]

    def counts(k):
        block = iota((KEYS, wide), 1) // KEYS
        total = f_ref[k, 0:KEYS, :]
        for j in range(1, wide // KEYS):
            total = jnp.where(block == j, f_ref[k, j * KEYS : (j + 1) * KEYS, :], total)
        return total

    def r_hot(meta, kind):
        row = jnp.broadcast_to(meta[:, kind : kind + 1, :], (srcs, part, LANES))
        lane, at = iota((part, LANES), 1), iota((part, LANES), 0)
        key = [
            jnp.sum(jnp.where((lane == at + w * part)[None], row, 0.0), axis=2, keepdims=True)
            for w in range(split_w)
        ]
        key = jnp.concatenate([x.reshape(srcs * part, 1) for x in key], 0)
        return key == key_in((m, LANES), 1)

    def joins(s_table, t_table, s_more, t_more, more, i):
        meta = meta_of(i)
        ra = r_hot(meta, 4)
        rb = r_hot(meta, 5)
        half = iota((m, LANES), 1) // KEYS
        ra16, rb16 = ra.astype(bf16), rb.astype(bf16)
        va, vb = mm(ra16, t_table), mm(rb16, s_table)
        pick = va[:, LANES : 2 * LANES] + va[:, 2 * LANES : 3 * LANES]
        scale = jnp.sum(jnp.where(rb, pick, 0.0), axis=1, keepdims=True)

        def sides(value, hot):
            both = (value[:, 0:LANES], jnp.where(hot, 0.0, -BIG))
            return [
                jnp.concatenate([jnp.where(half == w, x, 0.0).astype(bf16) for x in both], 1)
                for w in range(split_w)
            ]

        def one(of_s, of_t, j, acc):
            at = pl.ds(j * m, m)
            rows = held[pl.ds(j * srcs, srcs), 0 : 2 * cap, :]
            xs, matches = [], []
            for left, ref, start in ((of_s, s_ref, 0), (of_t, t_ref, cap)):
                x = rows[:, start : start + cap, :].reshape(m, LANES).T
                right = ref[at]
                for w in range(split_w):
                    xs.append(x[w * rows_of : (w + 1) * rows_of])
                    matches.append(jnp.maximum(mm_nt(right, left[w]), 0.0).astype(bf16))
            return acc + mm(jnp.concatenate(xs, 1), jnp.concatenate(matches, 0))

        def over(of_s, of_t, acc):
            step = functools.partial(one, of_s, of_t)
            return step(0, acc) if blocks == 1 else lax.fori_loop(0, blocks, step, acc)

        acc = over(sides(va, rb), sides(vb, ra), jnp.zeros((rows_of, m), f32))
        again = lambda x: over(sides(mm(ra16, t_more), rb), sides(mm(rb16, s_more), ra), x)
        acc = lax.cond(more, again, lambda x: x, acc)
        size = srcs * part
        acc = jnp.concatenate([acc[:, w * size : (w + 1) * size] for w in range(split_w)], 0).T
        factor = scale[0:size]
        for w in range(1, split_w):
            factor = jnp.where(
                iota((size, LANES), 1) < w * rows_of, factor, scale[w * size : (w + 1) * size]
            )
        out[pl.ds(i * srcs, srcs)] = (acc * factor).reshape(srcs, part, LANES)

    def each(step):
        if blocks == 1:
            step(0)
        else:
            pl.loop(0, blocks)(step)

    if blocks > 1:
        f_ref[...] = jnp.zeros_like(f_ref)
    each(tables)
    s_counts, t_counts = counts(0), counts(1)
    triangles = sum(mm_nt(t, s) for t in split(t_counts) for s in split(s_counts))
    scale = 1.0 / jnp.sqrt(1.0 + triangles)
    hi, _ = split(scale)
    middle, rest = split(scale - hi.astype(f32))

    def parts(count):
        count = count[:, 0:LANES]
        high = jnp.floor(count / EXACT) * EXACT
        return count - high, high

    def table(*columns):
        x = jnp.concatenate([c.astype(f32) for c in columns], 1).astype(bf16)
        return jnp.concatenate([x, jnp.zeros_like(x)], 0)

    s_low, s_high = parts(s_counts)
    t_low, t_high = parts(t_counts)
    each(
        functools.partial(
            joins,
            table(s_low),
            table(t_low, hi, middle, rest, jnp.zeros((KEYS, KEYS), f32)),
            table(s_high),
            table(t_high),
            jnp.maximum(jnp.max(s_high), jnp.max(t_high)) > 0.0,
        )
    )


def body(sizes, r_rows, r_keys, r_counts, s_rows, s_keys, s_counts, t_rows, t_keys, t_counts):
    n_a, n_b, n_c = sizes
    n = n_a * n_b * n_c
    cap = r_keys.shape[0] // r_counts.shape[0]
    width = r_rows.shape[1]
    srcs = max(512 // cap, 1)
    srcs = srcs if n % srcs == 0 else n
    total_slots = n * cap
    split_w = 2 if n_c % 2 == 0 and width == LANES and cap % 16 == 0 else 1
    wide = -(-n_c // 2) * LANES
    row = lambda x: x.reshape(1, x.shape[0])
    far = lambda x: pltpu.with_memory_space_constraint(x, pltpu.HBM)
    near = lambda x: pltpu.with_memory_space_constraint(x, pltpu.VMEM)
    params = pltpu.CompilerParams(vmem_limit_bytes=40 << 20)
    small = (row(s_keys), row(t_keys), row(r_keys), row(s_counts), row(t_counts), row(r_counts))
    groups = (s_rows.shape[0] // cap, t_rows.shape[0] // cap, r_rows.shape[0] // cap)
    blocked = [x.reshape(g, cap, width) for x, g in zip((s_rows, t_rows, r_rows), groups)]
    near_like = lambda x: pltpu.VMEM(x.shape, x.dtype)
    packed, r_kept = pl.pallas_call(
        functools.partial(pack_kernel, n_a, n_b, n_c, cap, split_w),
        in_specs=[pl.BlockSpec(memory_space=pltpu.HBM)] * 9,
        out_shape=(pltpu.VMEM((n, 2 * cap + META, width), bf16), near_like(blocked[2])),
        scratch_shapes=[near_like(x) for x in (*blocked[:2], *small)]
        + [pltpu.SemaphoreType.DMA((9,))],
        compiler_params=params,
        name="pack",
    )(*map(far, (*blocked, *small)))
    held = lax.all_to_all(packed, AXES, split_axis=0, concat_axis=0, tiled=True)
    shares = pl.pallas_call(
        functools.partial(join_kernel, n_c, cap, split_w, srcs),
        out_shape=pltpu.VMEM((n, cap // split_w, width), f32),
        scratch_shapes=[pltpu.VMEM((total_slots, 2 * LANES), bf16)] * 2
        + [pltpu.VMEM((2, wide, wide), f32)],
        compiler_params=params,
        name="join",
    )(near(held))
    back = lax.all_to_all(shares, AXES, split_axis=0, concat_axis=0, tiled=True)
    joined = pl.pallas_call(
        functools.partial(home_kernel, split_w),
        out_shape=jax.ShapeDtypeStruct(blocked[2].shape, bf16),
        compiler_params=params,
        name="home",
    )(near(back.reshape(n_a * n_b, n_c, cap // split_w, width)), near(r_kept))
    return joined.reshape(r_rows.shape)


def solution(mesh):
    rows, flat = P(AXES, None), P(AXES)
    sizes = tuple(mesh.shape[name] for name in AXES)
    return jax.shard_map(
        functools.partial(body, sizes),
        mesh=mesh,
        in_specs=(rows, flat, flat) * 3,
        out_specs=rows,
        check_vma=False,
    )
```

```python
import functools

import jax
import jax.numpy as jnp
from jax import lax
from jax.experimental import pallas as pl
from jax.experimental.pallas import tpu as pltpu
from jax.sharding import PartitionSpec as P

KEYS = 64
LANES = 128
META = 8
AXES = ("aa", "ba", "col")
f32 = jnp.float32
bf16 = jnp.bfloat16


def iota(shape, dim):
    return lax.broadcasted_iota(jnp.int32, shape, dim)


def split(x):
    hi = x.astype(bf16)
    return hi, (x - hi.astype(f32)).astype(bf16)


def mm(x, y):
    return lax.dot_general(x, y, (((1,), (0,)), ((), ())), preferred_element_type=f32)


def mm_nt(x, y):
    return lax.dot_general(x, y, (((1,), (1,)), ((), ())), preferred_element_type=f32)


def mm_tn(x, y):
    return lax.dot_general(x, y, (((0,), (0,)), ((), ())), preferred_element_type=f32)


def swap(x, y):
    half = x.shape[-1] // 2
    low = iota(x.shape, x.ndim - 1) < half
    turn = lambda v: pltpu.roll(v, half, v.ndim - 1)
    return jnp.where(low, x, turn(y)), jnp.where(low, turn(x), y)


def pack_kernel(
    n_a, n_b, n_c, cap, split_w,
    s_rows, t_rows, r_rows, s_keys, t_keys, r_keys, s_cnt, t_cnt, r_cnt,
    out, r_out,
    s_near, t_near,
    s_keys_near, t_keys_near, r_keys_near, s_cnt_near, t_cnt_near, r_cnt_near, sem,
):
    small = [
        pltpu.make_async_copy(far, near, sem.at[i])
        for i, (far, near) in enumerate(
            (
                (s_keys, s_keys_near),
                (t_keys, t_keys_near),
                (r_keys, r_keys_near),
                (s_cnt, s_cnt_near),
                (t_cnt, t_cnt_near),
                (r_cnt, r_cnt_near),
            )
        )
    ]
    rows = [
        pltpu.make_async_copy(far, near, sem.at[len(small) + i])
        for i, (far, near) in enumerate(((s_rows, s_near), (t_rows, t_near), (r_rows, r_out)))
    ]
    for copy in small + rows:
        copy.start()

    def halves(keys_ref, cnt_ref):
        keys = keys_ref[...]
        slots = keys.shape[1]
        groups = slots // cap
        spread = (iota((groups, slots), 1) // cap == iota((groups, slots), 0)).astype(bf16)
        cnt = jnp.broadcast_to(cnt_ref[...].astype(f32).astype(bf16), (8, groups))
        live = (iota((1, slots), 1) % cap).astype(f32) < mm(cnt, spread)[0:1]
        first = jnp.where(live, lax.div(keys, KEYS).astype(f32), -1.0)
        second = jnp.where(live, lax.rem(keys, KEYS).astype(f32), -1.0)
        return first, second

    def at(vec, start):
        row = vec[:, start // LANES * LANES : (start // LANES + 1) * LANES]
        return pltpu.roll(row, (LANES - start % LANES) % LANES, 1) if start % LANES else row

    for copy in small:
        copy.wait()
    sb, sc = halves(s_keys_near, s_cnt_near)
    ta, tc = halves(t_keys_near, t_cnt_near)
    ra, rb = halves(r_keys_near, r_cnt_near)
    seg = n_c * cap
    row = iota((META, LANES), 0)
    me = (lax.axis_index("aa") * n_b + lax.axis_index("ba")) * n_c + lax.axis_index("col")
    turn = lax.rem(me, LANES // cap) * cap

    def ring(vec, start):
        out = at(vec, start)
        size = seg
        while size < LANES:
            out = jnp.where(iota((1, LANES), 1) < size, out, pltpu.roll(out, size, 1))
            size *= 2
        return out

    s_meta = [(ring(sb, b * seg), ring(sc, b * seg)) for b in range(n_b)]
    t_meta = [(ring(ta, a * seg), ring(tc, a * seg)) for a in range(n_a)]
    for a in range(n_a):
        for b in range(n_b):
            meta = jnp.zeros((META, LANES), f32)
            for k, value in enumerate(s_meta[b] + t_meta[a]):
                meta = jnp.where(row == k, value, meta)
            r_at = (a * n_b + b) * cap
            for c in range(0, n_c, split_w):
                turned = pltpu.roll(meta, LANES - c * cap, 1) if c else meta
                for k, vec in ((4, ra), (5, rb)):
                    turned = jnp.where(row == k, at(vec, r_at), turned)
                turned = pltpu.roll(turned, turn, 1).astype(bf16)
                for w in range(split_w):
                    out[(a * n_b + b) * n_c + c + w, 2 * cap : 2 * cap + META, :] = turned
    for copy in rows:
        copy.wait()

    def parts(near, g):
        if split_w == 1:
            return (near[g],)
        pair = swap(near[g].astype(f32), near[g + 1].astype(f32))
        return tuple(x.astype(bf16) for x in pair)

    for c in range(0, n_c, split_w):
        for b in range(n_b):
            for w, part in enumerate(parts(s_near, b * n_c + c)):
                for a in range(n_a):
                    out[(a * n_b + b) * n_c + c + w, 0:cap, :] = part
        for a in range(n_a):
            for w, part in enumerate(parts(t_near, a * n_c + c)):
                for b in range(n_b):
                    out[(a * n_b + b) * n_c + c + w, cap : 2 * cap, :] = part


def home_kernel(split_w, shares, r_rows, out):
    groups, n_c, cap_w, width = shares.shape
    total = [shares[:, w] for w in range(split_w)]
    for c in range(split_w, n_c):
        total[c % split_w] = total[c % split_w] + shares[:, c]
    if split_w == 2:
        total = swap(*total)
    for w in range(split_w):
        at = pl.ds(w * cap_w, cap_w)
        out[:, at, :] = (r_rows[:, at, :].astype(f32) * total[w]).astype(bf16)


BIG = 2.0**15
EXACT = 256.0


def join_kernel(n_c, cap, split_w, srcs, held, out, s_ref, t_ref, f_ref):
    blocks = held.shape[0] // srcs
    m = srcs * cap
    ring = LANES // cap
    rows_of = LANES // split_w
    part = cap // split_w
    key = iota((KEYS, m), 0).astype(f32)

    def lanes(i, bucket):
        meta = held[pl.ds(i * srcs, srcs), 2 * cap : 2 * cap + META, :].astype(f32)
        block = iota((META, LANES), 1) // cap
        groups = []
        for g in range(0, srcs, ring):
            row = meta[g]
            for j in range(1, ring):
                row = jnp.where(block == (j + bucket) % ring, meta[g + j], row)
            groups.append(row)
        return jnp.concatenate(groups, 1)

    def hot(rows, kind):
        return rows[kind : kind + 1, :] == key

    def tables(i):
        counts, own = [], []
        for bucket in range(n_c):
            rows = lanes(i, bucket)
            for k in range(2):
                first, c = hot(rows, 2 * k).astype(bf16), hot(rows, 2 * k + 1).astype(bf16)
                counts.append(mm_nt(first, jnp.concatenate([c, c], 0)))
                if bucket < split_w:
                    own.append((c, first))
        empty = jnp.zeros((KEYS, m), bf16)
        for k, ref in enumerate((s_ref, t_ref)):
            mine = own[k::2] + [(empty, empty)] * (LANES // KEYS - split_w)
            both = [pair[0] for pair in mine] + [pair[1] for pair in mine]
            ref[pl.ds(i * m, m), :] = jnp.concatenate(both, 0).T
        return counts

    def joins(s_table, t_table, s_more, t_more, more, i):
        rows = lanes(i, 0)
        ra, rb = hot(rows, 4), hot(rows, 5)
        ra16, rb16 = ra.astype(bf16), rb.astype(bf16)
        va, vb = mm_tn(t_table, ra16), mm_tn(s_table, rb16)
        at = lambda k: va[LANES + k * KEYS : LANES + (k + 1) * KEYS]
        scale = jnp.sum(jnp.where(rb, at(0) + at(1) + at(2), 0.0), axis=0, keepdims=True)
        empty = jnp.zeros((KEYS, m), bf16)

        def sides(value, hot):
            value = value.astype(bf16)
            flag = jnp.where(hot, 0.0, -BIG).astype(bf16)

            def side(w):
                part = [empty] * (2 * LANES // KEYS)
                part[w] = value[w * KEYS : (w + 1) * KEYS]
                part[LANES // KEYS + w] = flag
                return jnp.concatenate(part, 0)

            return [side(w) for w in range(split_w)]

        def one(of_s, of_t, j, acc):
            at = pl.ds(j * m, m)
            rows = held[pl.ds(j * srcs, srcs), 0 : 2 * cap, :]
            xs, matches = [], []
            for left, ref, start in ((of_s, s_ref, 0), (of_t, t_ref, cap)):
                x = rows[:, start : start + cap, :].reshape(srcs // ring, ring, cap, LANES)
                turned = x
                for w in range(1, split_w):
                    shifted = jnp.concatenate([x[:, ring - w :], x[:, : ring - w]], 1)
                    turned = jnp.where(iota(x.shape, 3) < w * rows_of, turned, shifted)
                xs.append(turned.reshape(m, LANES).T)
                right = ref[at]
                for w in range(split_w):
                    matches.append(jnp.maximum(mm(right, left[w]), 0.0).astype(bf16))
            xs = [x[w * rows_of : (w + 1) * rows_of] for x in xs for w in range(split_w)]
            return acc + mm(jnp.concatenate(xs, 1), jnp.concatenate(matches, 0))

        def over(of_s, of_t, acc):
            step = functools.partial(one, of_s, of_t)
            return step(0, acc) if blocks == 1 else lax.fori_loop(0, blocks, step, acc)

        acc = over(sides(va, rb), sides(vb, ra), jnp.zeros((rows_of, m), f32))
        again = lambda x: over(sides(mm_tn(t_more, ra16), rb), sides(mm_tn(s_more, rb16), ra), x)
        acc = lax.cond(more, again, lambda x: x, acc) * scale
        acc = jnp.concatenate([acc] * split_w, 0).T.reshape(srcs, cap, LANES)
        result = acc[:, 0:part]
        for w in range(1, split_w):
            lane = iota((srcs, part, LANES), 2)
            result = jnp.where(lane < w * rows_of, result, acc[:, w * part : (w + 1) * part])
        out[pl.ds(i * srcs, srcs)] = result

    if blocks == 1:
        found = tables(0)
    else:
        f_ref[...] = jnp.zeros_like(f_ref)

        @pl.loop(0, blocks)
        def _(i):
            for k, count in enumerate(tables(i)):
                f_ref[k] += count

        found = [f_ref[k] for k in range(2 * n_c)]
    low = iota((KEYS, LANES), 1) < KEYS
    found += [jnp.zeros((KEYS, LANES), f32)] * (2 * (n_c % 2))
    counts = [
        [jnp.where(low, found[k + 2 * b], found[k + 2 * b + 2]) for b in range(0, n_c, 2)]
        for k in range(2)
    ]
    s_split, t_split = [split(jnp.concatenate(x, 1)) for x in counts]
    triangles = sum(mm_nt(t, s) for t in t_split for s in s_split)
    scale = 1.0 / jnp.sqrt(1.0 + triangles)
    hi, _ = split(scale)
    middle, rest = split(scale - hi.astype(f32))

    def parts(count):
        high = jnp.floor(count / EXACT) * EXACT
        return count - high, high

    def table(*columns):
        return jnp.concatenate([c.astype(f32) for c in columns], 1).astype(bf16)

    s_low, s_high = parts(counts[0][0])
    t_low, t_high = parts(counts[1][0])
    step = functools.partial(
        joins,
        table(s_low),
        table(t_low, hi, middle, rest, jnp.zeros((KEYS, KEYS), f32)),
        table(s_high),
        table(t_high),
        jnp.maximum(jnp.max(s_high), jnp.max(t_high)) > 0.0,
    )
    if blocks == 1:
        step(0)
    else:
        pl.loop(0, blocks)(step)


def body(sizes, r_rows, r_keys, r_counts, s_rows, s_keys, s_counts, t_rows, t_keys, t_counts):
    n_a, n_b, n_c = sizes
    n = n_a * n_b * n_c
    cap = r_keys.shape[0] // r_counts.shape[0]
    width = r_rows.shape[1]
    srcs = max(512 // cap, 1)
    srcs = srcs if n % srcs == 0 else n
    total_slots = n * cap
    split_w = 2 if n_c % 2 == 0 and width == LANES and cap % 16 == 0 else 1
    row = lambda x: x.reshape(1, x.shape[0])
    far = lambda x: pltpu.with_memory_space_constraint(x, pltpu.HBM)
    near = lambda x: pltpu.with_memory_space_constraint(x, pltpu.VMEM)
    params = pltpu.CompilerParams(vmem_limit_bytes=40 << 20)
    small = (row(s_keys), row(t_keys), row(r_keys), row(s_counts), row(t_counts), row(r_counts))
    groups = (s_rows.shape[0] // cap, t_rows.shape[0] // cap, r_rows.shape[0] // cap)
    blocked = [x.reshape(g, cap, width) for x, g in zip((s_rows, t_rows, r_rows), groups)]
    near_like = lambda x: pltpu.VMEM(x.shape, x.dtype)
    packed, r_kept = pl.pallas_call(
        functools.partial(pack_kernel, n_a, n_b, n_c, cap, split_w),
        in_specs=[pl.BlockSpec(memory_space=pltpu.HBM)] * 9,
        out_shape=(pltpu.VMEM((n, 2 * cap + META, width), bf16), near_like(blocked[2])),
        scratch_shapes=[near_like(x) for x in (*blocked[:2], *small)]
        + [pltpu.SemaphoreType.DMA((9,))],
        compiler_params=params,
        name="pack",
    )(*map(far, (*blocked, *small)))
    held = lax.all_to_all(packed, AXES, split_axis=0, concat_axis=0, tiled=True)
    shares = pl.pallas_call(
        functools.partial(join_kernel, n_c, cap, split_w, srcs),
        out_shape=pltpu.VMEM((n, cap // split_w, width), f32),
        scratch_shapes=[pltpu.VMEM((total_slots, 2 * LANES), bf16)] * 2
        + [pltpu.VMEM((2 * n_c, KEYS, LANES), f32)],
        compiler_params=params,
        name="join",
    )(near(held))
    back = lax.all_to_all(shares, AXES, split_axis=0, concat_axis=0, tiled=True)
    joined = pl.pallas_call(
        functools.partial(home_kernel, split_w),
        out_shape=jax.ShapeDtypeStruct(blocked[2].shape, bf16),
        compiler_params=params,
        name="home",
    )(near(back.reshape(n_a * n_b, n_c, cap // split_w, width)), near(r_kept))
    return joined.reshape(r_rows.shape)


def solution(mesh):
    rows, flat = P(AXES, None), P(AXES)
    sizes = tuple(mesh.shape[name] for name in AXES)
    return jax.shard_map(
        functools.partial(body, sizes),
        mesh=mesh,
        in_specs=(rows, flat, flat) * 3,
        out_specs=rows,
        check_vma=False,
    )
```

```python
import functools

import jax
import jax.numpy as jnp
from jax import lax
from jax.experimental import pallas as pl
from jax.experimental.pallas import tpu as pltpu
from jax.sharding import PartitionSpec as P

KEYS = 64
LANES = 128
META = 8
AXES = ("aa", "ba", "col")
f32 = jnp.float32
bf16 = jnp.bfloat16


def iota(shape, dim):
    return lax.broadcasted_iota(jnp.int32, shape, dim)


def split(x):
    hi = x.astype(bf16)
    return hi, (x - hi.astype(f32)).astype(bf16)


def mm(x, y):
    return lax.dot_general(x, y, (((1,), (0,)), ((), ())), preferred_element_type=f32)


def mm_nt(x, y):
    return lax.dot_general(x, y, (((1,), (1,)), ((), ())), preferred_element_type=f32)


def mm_tn(x, y):
    return lax.dot_general(x, y, (((0,), (0,)), ((), ())), preferred_element_type=f32)


def swap(x, y):
    half = x.shape[-1] // 2
    low = iota(x.shape, x.ndim - 1) < half
    turn = lambda v: pltpu.roll(v, half, v.ndim - 1)
    return jnp.where(low, x, turn(y)), jnp.where(low, turn(x), y)


def pack_kernel(
    n_a, n_b, n_c, cap, split_w,
    s_rows, t_rows, r_rows, s_keys, t_keys, r_keys, s_cnt, t_cnt, r_cnt,
    out, r_out,
    s_near, t_near,
    s_keys_near, t_keys_near, r_keys_near, s_cnt_near, t_cnt_near, r_cnt_near, sem,
):
    small = [
        pltpu.make_async_copy(far, near, sem.at[i])
        for i, (far, near) in enumerate(
            (
                (s_keys, s_keys_near),
                (t_keys, t_keys_near),
                (r_keys, r_keys_near),
                (s_cnt, s_cnt_near),
                (t_cnt, t_cnt_near),
                (r_cnt, r_cnt_near),
            )
        )
    ]
    rows = [
        pltpu.make_async_copy(far, near, sem.at[len(small) + i])
        for i, (far, near) in enumerate(((s_rows, s_near), (t_rows, t_near), (r_rows, r_out)))
    ]
    for copy in small + rows:
        copy.start()

    def halves(keys_ref, cnt_ref):
        keys = keys_ref[...]
        slots = keys.shape[1]
        groups = slots // cap
        spread = (iota((groups, slots), 1) // cap == iota((groups, slots), 0)).astype(bf16)
        cnt = jnp.broadcast_to(cnt_ref[...].astype(f32).astype(bf16), (8, groups))
        live = (iota((1, slots), 1) % cap).astype(f32) < mm(cnt, spread)[0:1]
        first = jnp.where(live, lax.div(keys, KEYS).astype(f32), -1.0)
        second = jnp.where(live, lax.rem(keys, KEYS).astype(f32), -1.0)
        return first, second

    def at(vec, start):
        row = vec[:, start // LANES * LANES : (start // LANES + 1) * LANES]
        return pltpu.roll(row, (LANES - start % LANES) % LANES, 1) if start % LANES else row

    for copy in small:
        copy.wait()
    sb, sc = halves(s_keys_near, s_cnt_near)
    ta, tc = halves(t_keys_near, t_cnt_near)
    ra, rb = halves(r_keys_near, r_cnt_near)
    seg = n_c * cap
    row = iota((META, LANES), 0)
    me = (lax.axis_index("aa") * n_b + lax.axis_index("ba")) * n_c + lax.axis_index("col")
    turn = lax.rem(me, LANES // cap) * cap

    def ring(vec, start):
        out = at(vec, start)
        size = seg
        while size < LANES:
            out = jnp.where(iota((1, LANES), 1) < size, out, pltpu.roll(out, size, 1))
            size *= 2
        return out

    s_meta = [(ring(sb, b * seg), ring(sc, b * seg)) for b in range(n_b)]
    t_meta = [(ring(ta, a * seg), ring(tc, a * seg)) for a in range(n_a)]
    for a in range(n_a):
        for b in range(n_b):
            meta = jnp.zeros((META, LANES), f32)
            for k, value in enumerate(s_meta[b] + t_meta[a]):
                meta = jnp.where(row == k, value, meta)
            r_at = (a * n_b + b) * cap
            for c in range(0, n_c, split_w):
                turned = pltpu.roll(meta, LANES - c * cap, 1) if c else meta
                for k, vec in ((4, ra), (5, rb)):
                    turned = jnp.where(row == k, at(vec, r_at), turned)
                turned = pltpu.roll(turned, turn, 1).astype(bf16)
                for w in range(split_w):
                    out[(a * n_b + b) * n_c + c + w, 2 * cap : 2 * cap + META, :] = turned
    for copy in rows:
        copy.wait()

    def parts(near, g):
        if split_w == 1:
            return (near[g],)
        pair = swap(near[g].astype(f32), near[g + 1].astype(f32))
        return tuple(x.astype(bf16) for x in pair)

    for c in range(0, n_c, split_w):
        for b in range(n_b):
            for w, part in enumerate(parts(s_near, b * n_c + c)):
                for a in range(n_a):
                    out[(a * n_b + b) * n_c + c + w, 0:cap, :] = part
        for a in range(n_a):
            for w, part in enumerate(parts(t_near, a * n_c + c)):
                for b in range(n_b):
                    out[(a * n_b + b) * n_c + c + w, cap : 2 * cap, :] = part


def home_kernel(split_w, shares, r_rows, out):
    groups, n_c, cap_w, width = shares.shape
    total = [shares[:, w] for w in range(split_w)]
    for c in range(split_w, n_c):
        total[c % split_w] = total[c % split_w] + shares[:, c]
    if split_w == 2:
        total = swap(*total)
    for w in range(split_w):
        at = pl.ds(w * cap_w, cap_w)
        out[:, at, :] = (r_rows[:, at, :].astype(f32) * total[w]).astype(bf16)


BIG = 2.0**15
EXACT = 256.0


def join_kernel(n_c, cap, split_w, srcs, held, out, s_ref, t_ref, f_ref):
    blocks = held.shape[0] // srcs
    m = srcs * cap
    ring = LANES // cap
    rows_of = LANES // split_w
    part = cap // split_w
    key = iota((KEYS, m), 0).astype(f32).astype(bf16)

    def lanes(i, bucket):
        meta = held[pl.ds(i * srcs, srcs), 2 * cap : 2 * cap + META, :].astype(f32)
        block = iota((META, LANES), 1) // cap
        groups = []
        for g in range(0, srcs, ring):
            row = meta[g]
            for j in range(1, ring):
                row = jnp.where(block == (j + bucket) % ring, meta[g + j], row)
            groups.append(row)
        return jnp.concatenate(groups, 1)

    def hot(rows, kind):
        return jnp.broadcast_to(rows[kind : kind + 1, :], (KEYS, m)).astype(bf16) == key

    def one_hot(rows, kind):
        return jnp.where(hot(rows, kind), jnp.ones_like(key), jnp.zeros_like(key))

    def tables(i):
        counts, own = [], []
        for bucket in range(n_c):
            rows = lanes(i, bucket)
            for k in range(2):
                first, c = one_hot(rows, 2 * k), one_hot(rows, 2 * k + 1)
                counts.append(mm_nt(first, jnp.concatenate([c, c], 0)))
                if bucket < split_w:
                    own.append((c, first))
        for k, ref in enumerate((s_ref, t_ref)):
            for w, pair in enumerate(own[k::2]):
                ref[w, pl.ds(i * m, m), :] = jnp.concatenate(pair, 0).T
        return counts

    def joins(s_table, t_table, s_more, t_more, more, i):
        rows = lanes(i, 0)
        ra, rb = hot(rows, 4), hot(rows, 5)
        ra16, rb16 = one_hot(rows, 4), one_hot(rows, 5)
        va, vb = mm_tn(t_table, ra16), mm_tn(s_table, rb16)
        at = lambda k: va[LANES + k * KEYS : LANES + (k + 1) * KEYS]
        scale = jnp.sum(jnp.where(rb16 > 0.5, at(0) + at(1) + at(2), 0.0), axis=0, keepdims=True)

        def sides(value, hot):
            value = value.astype(bf16)
            flag = jnp.where(hot, jnp.zeros_like(key), jnp.full_like(key, -BIG))
            return [
                jnp.concatenate([value[w * KEYS : (w + 1) * KEYS], flag], 0) for w in range(split_w)
            ]

        def one(of_s, of_t, j, acc):
            at = pl.ds(j * m, m)
            rows = held[pl.ds(j * srcs, srcs), 0 : 2 * cap, :]
            xs, matches = [], []
            for left, ref, start in ((of_s, s_ref, 0), (of_t, t_ref, cap)):
                x = rows[:, start : start + cap, :].reshape(srcs // ring, ring, cap, LANES)
                turned = x
                for w in range(1, split_w):
                    shifted = jnp.concatenate([x[:, ring - w :], x[:, : ring - w]], 1)
                    turned = jnp.where(iota(x.shape, 3) < w * rows_of, turned, shifted)
                xs.append(turned.reshape(m, LANES).T)
                for w in range(split_w):
                    matches.append(jnp.maximum(mm(ref[w, at], left[w]), 0.0).astype(bf16))
            xs = [x[w * rows_of : (w + 1) * rows_of] for x in xs for w in range(split_w)]
            return acc + mm(jnp.concatenate(xs, 1), jnp.concatenate(matches, 0))

        def over(of_s, of_t, acc):
            step = functools.partial(one, of_s, of_t)
            return step(0, acc) if blocks == 1 else lax.fori_loop(0, blocks, step, acc)

        acc = over(sides(va, rb), sides(vb, ra), jnp.zeros((rows_of, m), f32))
        again = lambda x: over(sides(mm_tn(t_more, ra16), rb), sides(mm_tn(s_more, rb16), ra), x)
        acc = lax.cond(more, again, lambda x: x, acc) * scale
        acc = jnp.concatenate([acc] * split_w, 0).T.reshape(srcs, cap, LANES)
        result = acc[:, 0:part]
        for w in range(1, split_w):
            lane = iota((srcs, part, LANES), 2)
            result = jnp.where(lane < w * rows_of, result, acc[:, w * part : (w + 1) * part])
        out[pl.ds(i * srcs, srcs)] = result

    if blocks == 1:
        found = tables(0)
    else:
        f_ref[...] = jnp.zeros_like(f_ref)

        @pl.loop(0, blocks)
        def _(i):
            for k, count in enumerate(tables(i)):
                f_ref[k] += count

        found = [f_ref[k] for k in range(2 * n_c)]
    low = iota((KEYS, LANES), 1) < KEYS
    found += [jnp.zeros((KEYS, LANES), f32)] * (2 * (n_c % 2))
    counts = [
        [jnp.where(low, found[k + 2 * b], found[k + 2 * b + 2]) for b in range(0, n_c, 2)]
        for k in range(2)
    ]
    s_split, t_split = [split(jnp.concatenate(x, 1)) for x in counts]
    triangles = sum(mm_nt(t, s) for t in t_split for s in s_split)
    scale = 1.0 / jnp.sqrt(1.0 + triangles)
    hi, _ = split(scale)
    middle, rest = split(scale - hi.astype(f32))

    def parts(count):
        high = jnp.floor(count / EXACT) * EXACT
        return count - high, high

    def table(*columns):
        return jnp.concatenate([c.astype(f32) for c in columns], 1).astype(bf16)

    s_low, s_high = parts(counts[0][0])
    t_low, t_high = parts(counts[1][0])
    step = functools.partial(
        joins,
        table(s_low),
        table(t_low, hi, middle, rest, jnp.zeros((KEYS, KEYS), f32)),
        table(s_high),
        table(t_high),
        jnp.maximum(jnp.max(s_high), jnp.max(t_high)) > 0.0,
    )
    if blocks == 1:
        step(0)
    else:
        pl.loop(0, blocks)(step)


def body(sizes, r_rows, r_keys, r_counts, s_rows, s_keys, s_counts, t_rows, t_keys, t_counts):
    n_a, n_b, n_c = sizes
    n = n_a * n_b * n_c
    cap = r_keys.shape[0] // r_counts.shape[0]
    width = r_rows.shape[1]
    srcs = max(512 // cap, 1)
    srcs = srcs if n % srcs == 0 else n
    total_slots = n * cap
    split_w = 2 if n_c % 2 == 0 and width == LANES and cap % 16 == 0 else 1
    row = lambda x: x.reshape(1, x.shape[0])
    far = lambda x: pltpu.with_memory_space_constraint(x, pltpu.HBM)
    near = lambda x: pltpu.with_memory_space_constraint(x, pltpu.VMEM)
    params = pltpu.CompilerParams(vmem_limit_bytes=40 << 20)
    small = (row(s_keys), row(t_keys), row(r_keys), row(s_counts), row(t_counts), row(r_counts))
    groups = (s_rows.shape[0] // cap, t_rows.shape[0] // cap, r_rows.shape[0] // cap)
    blocked = [x.reshape(g, cap, width) for x, g in zip((s_rows, t_rows, r_rows), groups)]
    near_like = lambda x: pltpu.VMEM(x.shape, x.dtype)
    packed, r_kept = pl.pallas_call(
        functools.partial(pack_kernel, n_a, n_b, n_c, cap, split_w),
        in_specs=[pl.BlockSpec(memory_space=pltpu.HBM)] * 9,
        out_shape=(pltpu.VMEM((n, 2 * cap + META, width), bf16), near_like(blocked[2])),
        scratch_shapes=[near_like(x) for x in (*blocked[:2], *small)]
        + [pltpu.SemaphoreType.DMA((9,))],
        compiler_params=params,
        name="pack",
    )(*map(far, (*blocked, *small)))
    held = lax.all_to_all(packed, AXES, split_axis=0, concat_axis=0, tiled=True)
    shares = pl.pallas_call(
        functools.partial(join_kernel, n_c, cap, split_w, srcs),
        out_shape=pltpu.VMEM((n, cap // split_w, width), f32),
        scratch_shapes=[pltpu.VMEM((split_w, total_slots, LANES), bf16)] * 2
        + [pltpu.VMEM((2 * n_c, KEYS, LANES), f32)],
        compiler_params=params,
        name="join",
    )(near(held))
    back = lax.all_to_all(shares, AXES, split_axis=0, concat_axis=0, tiled=True)
    joined = pl.pallas_call(
        functools.partial(home_kernel, split_w),
        out_shape=jax.ShapeDtypeStruct(blocked[2].shape, bf16),
        compiler_params=params,
        name="home",
    )(near(back.reshape(n_a * n_b, n_c, cap // split_w, width)), near(r_kept))
    return joined.reshape(r_rows.shape)


def solution(mesh):
    rows, flat = P(AXES, None), P(AXES)
    sizes = tuple(mesh.shape[name] for name in AXES)
    return jax.shard_map(
        functools.partial(body, sizes),
        mesh=mesh,
        in_specs=(rows, flat, flat) * 3,
        out_specs=rows,
        check_vma=False,
    )
```

```python
import functools

import jax
import jax.numpy as jnp
from jax import lax
from jax.experimental import pallas as pl
from jax.experimental.pallas import tpu as pltpu
from jax.sharding import PartitionSpec as P

KEYS = 64
LANES = 128
META = 8
AXES = ("aa", "ba", "col")
f32 = jnp.float32
bf16 = jnp.bfloat16


def iota(shape, dim):
    return lax.broadcasted_iota(jnp.int32, shape, dim)


def split(x):
    hi = x.astype(bf16)
    return hi, (x - hi.astype(f32)).astype(bf16)


def mm(x, y):
    return lax.dot_general(x, y, (((1,), (0,)), ((), ())), preferred_element_type=f32)


def mm_nt(x, y):
    return lax.dot_general(x, y, (((1,), (1,)), ((), ())), preferred_element_type=f32)


def mm_tn(x, y):
    return lax.dot_general(x, y, (((0,), (0,)), ((), ())), preferred_element_type=f32)


def swap(x, y):
    half = x.shape[-1] // 2
    low = iota(x.shape, x.ndim - 1) < half
    turn = lambda v: pltpu.roll(v, half, v.ndim - 1)
    return jnp.where(low, x, turn(y)), jnp.where(low, turn(x), y)


def pack_kernel(
    n_a, n_b, n_c, cap, split_w,
    s_rows, t_rows, r_rows, s_keys, t_keys, r_keys, s_cnt, t_cnt, r_cnt,
    out, r_out,
    s_near, t_near,
    s_keys_near, t_keys_near, r_keys_near, s_cnt_near, t_cnt_near, r_cnt_near, sem,
):
    small = [
        pltpu.make_async_copy(far, near, sem.at[i])
        for i, (far, near) in enumerate(
            (
                (s_keys, s_keys_near),
                (t_keys, t_keys_near),
                (r_keys, r_keys_near),
                (s_cnt, s_cnt_near),
                (t_cnt, t_cnt_near),
                (r_cnt, r_cnt_near),
            )
        )
    ]
    rows = [
        pltpu.make_async_copy(far, near, sem.at[len(small) + i])
        for i, (far, near) in enumerate(((s_rows, s_near), (t_rows, t_near), (r_rows, r_out)))
    ]
    for copy in small + rows:
        copy.start()

    def halves(keys_ref, cnt_ref):
        keys = keys_ref[...]
        slots = keys.shape[1]
        groups = slots // cap
        spread = (iota((groups, slots), 1) // cap == iota((groups, slots), 0)).astype(bf16)
        cnt = jnp.broadcast_to(cnt_ref[...].astype(f32).astype(bf16), (8, groups))
        live = (iota((1, slots), 1) % cap).astype(f32) < mm(cnt, spread)[0:1]
        first = jnp.where(live, lax.div(keys, KEYS).astype(f32), -1.0)
        second = jnp.where(live, lax.rem(keys, KEYS).astype(f32), -1.0)
        return first, second

    def at(vec, start):
        row = vec[:, start // LANES * LANES : (start // LANES + 1) * LANES]
        return pltpu.roll(row, (LANES - start % LANES) % LANES, 1) if start % LANES else row

    for copy in small:
        copy.wait()
    sb, sc = halves(s_keys_near, s_cnt_near)
    ta, tc = halves(t_keys_near, t_cnt_near)
    ra, rb = halves(r_keys_near, r_cnt_near)
    seg = n_c * cap
    row = iota((META, LANES), 0)
    me = (lax.axis_index("aa") * n_b + lax.axis_index("ba")) * n_c + lax.axis_index("col")
    turn = lax.rem(me, LANES // cap) * cap

    def ring(vec, start):
        out = at(vec, start)
        size = seg
        while size < LANES:
            out = jnp.where(iota((1, LANES), 1) < size, out, pltpu.roll(out, size, 1))
            size *= 2
        return out

    s_meta = [(ring(sb, b * seg), ring(sc, b * seg)) for b in range(n_b)]
    t_meta = [(ring(ta, a * seg), ring(tc, a * seg)) for a in range(n_a)]
    for a in range(n_a):
        for b in range(n_b):
            meta = jnp.zeros((META, LANES), f32)
            for k, value in enumerate(s_meta[b] + t_meta[a]):
                meta = jnp.where(row == k, value, meta)
            r_at = (a * n_b + b) * cap
            for c in range(0, n_c, split_w):
                turned = pltpu.roll(meta, LANES - c * cap, 1) if c else meta
                for k, vec in ((4, ra), (5, rb)):
                    turned = jnp.where(row == k, at(vec, r_at), turned)
                turned = pltpu.roll(turned, turn, 1).astype(bf16)
                for w in range(split_w):
                    out[(a * n_b + b) * n_c + c + w, 2 * cap : 2 * cap + META, :] = turned
    for copy in rows:
        copy.wait()

    def parts(near, g):
        if split_w == 1:
            return (near[g],)
        pair = swap(near[g].astype(f32), near[g + 1].astype(f32))
        return tuple(x.astype(bf16) for x in pair)

    for c in range(0, n_c, split_w):
        for b in range(n_b):
            for w, part in enumerate(parts(s_near, b * n_c + c)):
                for a in range(n_a):
                    out[(a * n_b + b) * n_c + c + w, 0:cap, :] = part
        for a in range(n_a):
            for w, part in enumerate(parts(t_near, a * n_c + c)):
                for b in range(n_b):
                    out[(a * n_b + b) * n_c + c + w, cap : 2 * cap, :] = part


def home_kernel(split_w, shares, r_rows, out):
    groups, n_c, cap_w, width = shares.shape
    total = [shares[:, w] for w in range(split_w)]
    for c in range(split_w, n_c):
        total[c % split_w] = total[c % split_w] + shares[:, c]
    if split_w == 2:
        total = swap(*total)
    for w in range(split_w):
        at = pl.ds(w * cap_w, cap_w)
        out[:, at, :] = (r_rows[:, at, :].astype(f32) * total[w]).astype(bf16)


BIG = 2.0**15
EXACT = 256.0


def join_kernel(n_c, cap, split_w, srcs, held, out, s_ref, t_ref, own_ref, all_ref):
    blocks = held.shape[0] // srcs
    m = srcs * cap
    ring = LANES // cap
    rows_of = LANES // split_w
    part = cap // split_w
    key = iota((KEYS, m), 0).astype(f32).astype(bf16)

    def lanes(i, bucket):
        meta = held[pl.ds(i * srcs, srcs), 2 * cap : 2 * cap + META, :].astype(f32)
        block = iota((META, LANES), 1) // cap
        groups = []
        for g in range(0, srcs, ring):
            row = meta[g]
            for j in range(1, ring):
                row = jnp.where(block == (j + bucket) % ring, meta[g + j], row)
            groups.append(row)
        return jnp.concatenate(groups, 1)

    def hot_of(rows, kind):
        return jnp.broadcast_to(rows[kind : kind + 1, :], (KEYS, m)).astype(bf16) == key

    def one_hot(rows, kind):
        return jnp.where(hot_of(rows, kind), jnp.ones_like(key), jnp.zeros_like(key))

    def stack(i, kind, buckets):
        return jnp.concatenate([one_hot(lanes(i, bucket), kind) for bucket in buckets], 0)

    own = range(split_w)

    def own_counts(i):
        counts = []
        for k, ref in enumerate((s_ref, t_ref)):
            first, c = stack(i, 2 * k, own), stack(i, 2 * k + 1, own)
            counts.append(mm_nt(c, first))
            for w in own:
                at = slice(w * KEYS, (w + 1) * KEYS)
                ref[w, pl.ds(i * m, m), :] = jnp.concatenate([c[at], first[at]], 0).T
        return counts

    def all_counts(i):
        every = range(n_c)
        return [mm_nt(stack(i, 2 * k, every), stack(i, 2 * k + 1, every)) for k in range(2)]

    def tables(own_found):
        found = []
        for count in own_found:
            same = iota(count.shape, 0) // KEYS == iota(count.shape, 1) // KEYS
            count = jnp.where(same, count, 0.0)
            high = jnp.floor(count / EXACT) * EXACT
            found.append((count - high, high))
        more = jnp.maximum(jnp.max(found[0][1]), jnp.max(found[1][1])) > 0.0
        return [(low.astype(bf16), high.astype(bf16)) for low, high in found], more

    def halves_of(all_found):
        halves = []
        for count in all_found:
            block = iota((KEYS, count.shape[1]), 1) // KEYS
            total = count[0:KEYS]
            for b in range(1, n_c):
                total = jnp.where(block == b, count[b * KEYS : (b + 1) * KEYS], total)
            halves.append(split(total))
        return halves

    def scales(halves):
        triangles = sum(mm_nt(s, t) for s in halves[0] for t in halves[1])
        scale = 1.0 / jnp.sqrt(1.0 + triangles)
        hi, _ = split(scale)
        middle, rest = split(scale - hi.astype(f32))
        return jnp.concatenate([hi, middle, rest], 0)

    def joins(i, found, more, between=()):
        rows = lanes(i, 0)
        ra, rb = [jnp.concatenate([one_hot(rows, k)] * split_w, 0) for k in (4, 5)]
        (s_low, s_high), (t_low, t_high) = found

        def sides(table, hot, kind_flag):
            value = mm(table, hot).astype(bf16)
            flag = jnp.where(hot_of(rows, kind_flag), jnp.zeros_like(key), jnp.full_like(key, -BIG))
            return [jnp.concatenate([value[w * KEYS : (w + 1) * KEYS], flag], 0) for w in own]

        def one(of_s, of_t, between, j, acc):
            at = pl.ds(j * m, m)
            rows = held[pl.ds(j * srcs, srcs), 0 : 2 * cap, :]
            xs, matches = [], []
            for left, ref, start in ((of_s, s_ref, 0), (of_t, t_ref, cap)):
                x = rows[:, start : start + cap, :].reshape(srcs // ring, ring, cap, LANES)
                turned = x
                for w in range(1, split_w):
                    shifted = jnp.concatenate([x[:, ring - w :], x[:, : ring - w]], 1)
                    turned = jnp.where(iota(x.shape, 3) < w * rows_of, turned, shifted)
                xs.append(turned.reshape(m, LANES).T)
                for w in own:
                    if len(matches) in between:
                        between[len(matches)]()
                    matches.append(jnp.maximum(mm(ref[w, at], left[w]), 0.0).astype(bf16))
            xs = [x[w * rows_of : (w + 1) * rows_of] for x in xs for w in own]
            return acc + mm(jnp.concatenate(xs, 1), jnp.concatenate(matches, 0))

        def over(of_s, of_t, acc, between=()):
            step = functools.partial(one, of_s, of_t, between)
            return step(0, acc) if blocks == 1 else lax.fori_loop(0, blocks, step, acc)

        acc = over(sides(t_low, ra, 5), sides(s_low, rb, 4), jnp.zeros((rows_of, m), f32), between)
        again = lambda x: over(sides(t_high, ra, 5), sides(s_high, rb, 4), x)
        return acc, lambda x: lax.cond(more, again, lambda x: x, x)

    def factor(i, table):
        rows = lanes(i, 0)
        at = mm(table, one_hot(rows, 4))
        at = at[0:KEYS] + at[KEYS : 2 * KEYS] + at[2 * KEYS : 3 * KEYS]
        return jnp.sum(jnp.where(one_hot(rows, 5) > 0.5, at, 0.0), axis=0, keepdims=True)

    def finish(i, acc, by):
        acc = acc * by
        acc = jnp.concatenate([acc] * split_w, 0).T.reshape(srcs, cap, LANES)
        result = acc[:, 0:part]
        for w in range(1, split_w):
            lane = iota((srcs, part, LANES), 2)
            result = jnp.where(lane < w * rows_of, result, acc[:, w * part : (w + 1) * part])
        out[pl.ds(i * srcs, srcs)] = result

    if blocks == 1:
        kept = {}
        found = tables(own_counts(0))
        halves = halves_of(all_counts(0))
        between = {
            0: lambda: kept.update(table=scales(halves)),
            split_w: lambda: kept.update(by=factor(0, kept["table"])),
        }
        acc, rest = joins(0, *found, between)
        finish(0, rest(acc), kept["by"])
        return

    own_ref[...] = jnp.zeros_like(own_ref)
    all_ref[...] = jnp.zeros_like(all_ref)

    @pl.loop(0, blocks)
    def _(i):
        for k, (mine, every) in enumerate(zip(own_counts(i), all_counts(i))):
            own_ref[k] += mine
            all_ref[k] += every

    found, more = tables([own_ref[0], own_ref[1]])
    table = scales(halves_of([all_ref[0], all_ref[1]]))

    @pl.loop(0, blocks)
    def _(i):
        acc, rest = joins(i, found, more)
        finish(i, rest(acc), factor(i, table))


def body(sizes, r_rows, r_keys, r_counts, s_rows, s_keys, s_counts, t_rows, t_keys, t_counts):
    n_a, n_b, n_c = sizes
    n = n_a * n_b * n_c
    cap = r_keys.shape[0] // r_counts.shape[0]
    width = r_rows.shape[1]
    srcs = max(512 // cap, 1)
    srcs = srcs if n % srcs == 0 else n
    total_slots = n * cap
    split_w = 2 if n_c % 2 == 0 and width == LANES and cap % 16 == 0 else 1
    row = lambda x: x.reshape(1, x.shape[0])
    far = lambda x: pltpu.with_memory_space_constraint(x, pltpu.HBM)
    near = lambda x: pltpu.with_memory_space_constraint(x, pltpu.VMEM)
    params = pltpu.CompilerParams(vmem_limit_bytes=40 << 20)
    small = (row(s_keys), row(t_keys), row(r_keys), row(s_counts), row(t_counts), row(r_counts))
    groups = (s_rows.shape[0] // cap, t_rows.shape[0] // cap, r_rows.shape[0] // cap)
    blocked = [x.reshape(g, cap, width) for x, g in zip((s_rows, t_rows, r_rows), groups)]
    near_like = lambda x: pltpu.VMEM(x.shape, x.dtype)
    packed, r_kept = pl.pallas_call(
        functools.partial(pack_kernel, n_a, n_b, n_c, cap, split_w),
        in_specs=[pl.BlockSpec(memory_space=pltpu.HBM)] * 9,
        out_shape=(pltpu.VMEM((n, 2 * cap + META, width), bf16), near_like(blocked[2])),
        scratch_shapes=[near_like(x) for x in (*blocked[:2], *small)]
        + [pltpu.SemaphoreType.DMA((9,))],
        compiler_params=params,
        name="pack",
    )(*map(far, (*blocked, *small)))
    held = lax.all_to_all(packed, AXES, split_axis=0, concat_axis=0, tiled=True)
    shares = pl.pallas_call(
        functools.partial(join_kernel, n_c, cap, split_w, srcs),
        out_shape=pltpu.VMEM((n, cap // split_w, width), f32),
        scratch_shapes=[pltpu.VMEM((split_w, total_slots, LANES), bf16)] * 2
        + [
            pltpu.VMEM((2, split_w * KEYS, split_w * KEYS), f32),
            pltpu.VMEM((2, n_c * KEYS, n_c * KEYS), f32),
        ],
        compiler_params=params,
        name="join",
    )(near(held))
    back = lax.all_to_all(shares, AXES, split_axis=0, concat_axis=0, tiled=True)
    joined = pl.pallas_call(
        functools.partial(home_kernel, split_w),
        out_shape=jax.ShapeDtypeStruct(blocked[2].shape, bf16),
        compiler_params=params,
        name="home",
    )(near(back.reshape(n_a * n_b, n_c, cap // split_w, width)), near(r_kept))
    return joined.reshape(r_rows.shape)


def solution(mesh):
    rows, flat = P(AXES, None), P(AXES)
    sizes = tuple(mesh.shape[name] for name in AXES)
    return jax.shard_map(
        functools.partial(body, sizes),
        mesh=mesh,
        in_specs=(rows, flat, flat) * 3,
        out_specs=rows,
        check_vma=False,
    )
```

```python
import functools

import jax
import jax.numpy as jnp
from jax import lax
from jax.experimental import pallas as pl
from jax.experimental.pallas import tpu as pltpu
from jax.sharding import PartitionSpec as P

KEYS = 64
LANES = 128
TILE = 4
AXES = ("aa", "ba", "col")
f32 = jnp.float32
bf16 = jnp.bfloat16


def iota(shape, dim):
    return lax.broadcasted_iota(jnp.int32, shape, dim)


def split(x):
    hi = x.astype(bf16)
    return hi, (x - hi.astype(f32)).astype(bf16)


def mm(x, y):
    return lax.dot_general(x, y, (((1,), (0,)), ((), ())), preferred_element_type=f32)


def mm_nt(x, y):
    return lax.dot_general(x, y, (((1,), (1,)), ((), ())), preferred_element_type=f32)


def mm_tn(x, y):
    return lax.dot_general(x, y, (((0,), (0,)), ((), ())), preferred_element_type=f32)


def swap(x, y):
    half = x.shape[-1] // 2
    low = iota(x.shape, x.ndim - 1) < half
    turn = lambda v: pltpu.roll(v, half, v.ndim - 1)
    return jnp.where(low, x, turn(y)), jnp.where(low, turn(x), y)


def pack_kernel(
    n_a, n_b, n_c, cap, split_w,
    s_rows, t_rows, r_rows, s_keys, t_keys, r_keys, s_cnt, t_cnt, r_cnt,
    out, r_out,
    s_near, t_near,
    s_keys_near, t_keys_near, r_keys_near, s_cnt_near, t_cnt_near, r_cnt_near, sem,
):
    small = [
        pltpu.make_async_copy(far, near, sem.at[i])
        for i, (far, near) in enumerate(
            (
                (s_keys, s_keys_near),
                (t_keys, t_keys_near),
                (r_keys, r_keys_near),
                (s_cnt, s_cnt_near),
                (t_cnt, t_cnt_near),
                (r_cnt, r_cnt_near),
            )
        )
    ]
    rows = [
        pltpu.make_async_copy(far, near, sem.at[len(small) + i])
        for i, (far, near) in enumerate(((s_rows, s_near), (t_rows, t_near), (r_rows, r_out)))
    ]
    for copy in small + rows:
        copy.start()

    def halves(keys_ref, cnt_ref):
        keys = keys_ref[...]
        slots = keys.shape[1]
        groups = slots // cap
        spread = (iota((groups, slots), 1) // cap == iota((groups, slots), 0)).astype(bf16)
        cnt = jnp.broadcast_to(cnt_ref[...].astype(f32).astype(bf16), (8, groups))
        live = (iota((1, slots), 1) % cap).astype(f32) < mm(cnt, spread)[0:1]
        first = jnp.where(live, lax.div(keys, KEYS).astype(f32), -1.0)
        second = jnp.where(live, lax.rem(keys, KEYS).astype(f32), -1.0)
        return first, second

    def at(vec, start):
        row = vec[:, start // LANES * LANES : (start // LANES + 1) * LANES]
        return pltpu.roll(row, (LANES - start % LANES) % LANES, 1) if start % LANES else row

    for copy in small:
        copy.wait()
    sb, sc = halves(s_keys_near, s_cnt_near)
    ta, tc = halves(t_keys_near, t_cnt_near)
    ra, rb = halves(r_keys_near, r_cnt_near)
    seg = n_c * cap
    tiles = out.shape[0] // (n_a * n_b * n_c)
    meta_rows = tiles * TILE - 2 * cap
    row = iota((meta_rows, LANES), 0)
    lane = iota((1, LANES), 1)
    me = (lax.axis_index("aa") * n_b + lax.axis_index("ba")) * n_c + lax.axis_index("col")
    turn = lax.rem(me, n_c) * cap

    def put(d, start, value):
        for t in range(value.shape[0] // TILE):
            out[d * tiles + start // TILE + t] = value[t * TILE : (t + 1) * TILE]

    def pairs(first, second, start):
        first, second = at(first, start), at(second, start)
        if seg == LANES:
            return [first, second]
        return [jnp.where(lane < seg, first, pltpu.roll(second, seg, 1))]

    def repeated(first, second):
        slots = first.shape[1]
        groups = slots // cap
        mine = iota((groups, slots), 1) // cap == iota((groups, slots), 0)
        same = iota((slots, LANES), 0) % cap == iota((slots, LANES), 1) % cap
        low = iota((slots, LANES), 1) < seg
        spread = lambda x, to: mm(jnp.where(mine, x, 0.0).astype(bf16), to.astype(bf16))
        if seg == LANES:
            return [spread(first, same), spread(second, same)]
        return [spread(first, same & low) + spread(second, same & ~low)]

    def turned(meta, by):
        if seg == LANES:
            return pltpu.roll(meta, by, 1)
        return jnp.where(
            iota(meta.shape, 1) % seg >= by, pltpu.roll(meta, by, 1), pltpu.roll(meta, by + seg, 1)
        )

    s_meta = [pairs(sb, sc, b * seg) for b in range(n_b)]
    t_meta = [pairs(ta, tc, a * seg) for a in range(n_a)]
    r_meta = repeated(ra, rb)
    for a in range(n_a):
        for b in range(n_b):
            g = a * n_b + b
            meta = jnp.zeros((meta_rows, LANES), f32)
            for k, value in enumerate(s_meta[b] + t_meta[a] + [x[g : g + 1] for x in r_meta]):
                meta = jnp.where(row == k, value, meta)
            for c in range(0, n_c, split_w):
                part = turned(meta, lax.rem(turn + seg - c * cap, seg)).astype(bf16)
                for w in range(split_w):
                    put(g * n_c + c + w, 2 * cap, part)
    for copy in rows:
        copy.wait()

    def parts(near, g):
        if split_w == 1:
            return (near[g],)
        pair = swap(near[g].astype(f32), near[g + 1].astype(f32))
        return tuple(x.astype(bf16) for x in pair)

    for c in range(0, n_c, split_w):
        for b in range(n_b):
            for w, part in enumerate(parts(s_near, b * n_c + c)):
                for a in range(n_a):
                    put((a * n_b + b) * n_c + c + w, 0, part)
        for a in range(n_a):
            for w, part in enumerate(parts(t_near, a * n_c + c)):
                for b in range(n_b):
                    put((a * n_b + b) * n_c + c + w, cap, part)


def home_kernel(split_w, shares, r_rows, out):
    groups, n_c, cap_w, width = shares.shape
    total = [shares[:, w] for w in range(split_w)]
    for c in range(split_w, n_c):
        total[c % split_w] = total[c % split_w] + shares[:, c]
    if split_w == 2:
        total = swap(*total)
    for w in range(split_w):
        at = pl.ds(w * cap_w, cap_w)
        out[:, at, :] = (r_rows[:, at, :].astype(f32) * total[w]).astype(bf16)


BIG = 2.0**15
EXACT = 256.0


def join_kernel(n_c, cap, split_w, srcs, tiles, held, out, s_ref, t_ref, own_ref, all_ref):
    blocks = held.shape[0] // (srcs * tiles)
    m = srcs * cap
    seg = n_c * cap
    rows_of = LANES // split_w
    part = cap // split_w
    key = iota((KEYS, m), 0).astype(f32).astype(bf16)

    def block_of(i):
        return held[pl.ds(i * srcs * tiles, srcs * tiles)].reshape(srcs, tiles, TILE, LANES)

    def lanes(i, bucket):
        meta = block_of(i)[:, 2 * cap // TILE :].astype(f32)
        meta = meta.reshape(srcs, meta.shape[1] * TILE, LANES)
        block = iota(meta.shape[1:], 1) % seg // cap
        groups = []
        for g in range(0, srcs, n_c):
            row = meta[g]
            for j in range(1, n_c):
                row = jnp.where(block == (j + bucket) % n_c, meta[g + j], row)
            groups.append(row)
        if seg == LANES:
            rows = jnp.concatenate(groups, 1)
            return [rows[k : k + 1] for k in range(6)]
        low = iota(meta.shape[1:], 1) < seg
        swapped = [
            (jnp.where(low, x, pltpu.roll(y, seg, 1)), jnp.where(low, pltpu.roll(x, seg, 1), y))
            for x, y in zip(groups[0::2], groups[1::2])
        ]
        both = [jnp.concatenate(x, 1) for x in zip(*swapped)]
        return [both[k % 2][k // 2 : k // 2 + 1] for k in range(6)]

    def hot_of(rows, kind):
        return jnp.broadcast_to(rows[kind], (KEYS, m)).astype(bf16) == key

    def one_hot(rows, kind):
        return jnp.where(hot_of(rows, kind), jnp.ones_like(key), jnp.zeros_like(key))

    def stack(i, kind, buckets):
        return jnp.concatenate([one_hot(lanes(i, bucket), kind) for bucket in buckets], 0)

    own = range(split_w)

    def own_counts(i):
        counts = []
        for k, ref in enumerate((s_ref, t_ref)):
            first, c = stack(i, 2 * k, own), stack(i, 2 * k + 1, own)
            counts.append(mm_nt(c, first))
            for w in own:
                at = slice(w * KEYS, (w + 1) * KEYS)
                ref[w, pl.ds(i * m, m), :] = jnp.concatenate([c[at], first[at]], 0).T
        return counts

    def all_counts(i):
        every = range(n_c)
        return [mm_nt(stack(i, 2 * k, every), stack(i, 2 * k + 1, every)) for k in range(2)]

    def tables(own_found):
        found = []
        for count in own_found:
            same = iota(count.shape, 0) // KEYS == iota(count.shape, 1) // KEYS
            count = jnp.where(same, count, 0.0)
            high = jnp.floor(count / EXACT) * EXACT
            found.append((count - high, high))
        more = jnp.maximum(jnp.max(found[0][1]), jnp.max(found[1][1])) > 0.0
        return [(low.astype(bf16), high.astype(bf16)) for low, high in found], more

    def halves_of(all_found):
        halves = []
        for count in all_found:
            block = iota((KEYS, count.shape[1]), 1) // KEYS
            total = count[0:KEYS]
            for b in range(1, n_c):
                total = jnp.where(block == b, count[b * KEYS : (b + 1) * KEYS], total)
            halves.append(split(total))
        return halves

    def scales(halves):
        triangles = sum(mm_nt(s, t) for s in halves[0] for t in halves[1])
        scale = 1.0 / jnp.sqrt(1.0 + triangles)
        hi, _ = split(scale)
        middle, rest = split(scale - hi.astype(f32))
        return jnp.concatenate([hi, middle, rest], 0)

    def joins(i, found, more, between=()):
        rows = lanes(i, 0)
        ra, rb = [jnp.concatenate([one_hot(rows, k)] * split_w, 0) for k in (4, 5)]
        (s_low, s_high), (t_low, t_high) = found

        def sides(table, hot, kind_flag):
            value = mm(table, hot).astype(bf16)
            flag = jnp.where(hot_of(rows, kind_flag), jnp.zeros_like(key), jnp.full_like(key, -BIG))
            return [jnp.concatenate([value[w * KEYS : (w + 1) * KEYS], flag], 0) for w in own]

        def one(of_s, of_t, between, j, acc):
            at = pl.ds(j * m, m)
            rows = block_of(j)
            xs, matches = [], []
            for left, ref, start in ((of_s, s_ref, 0), (of_t, t_ref, cap)):
                x = rows[:, start // TILE : (start + cap) // TILE]
                x = x.reshape(srcs // n_c, n_c, cap, LANES)
                turned = x.reshape(m, LANES)
                for w in range(1, split_w):
                    shifted = jnp.concatenate([x[:, n_c - w :], x[:, : n_c - w]], 1).reshape(m, LANES)
                    turned = jnp.concatenate([turned[:, : w * rows_of], shifted[:, w * rows_of :]], 1)
                xs.append(turned.T)
                for w in own:
                    if len(matches) in between:
                        between[len(matches)]()
                    matches.append(jnp.maximum(mm(ref[w, at], left[w]), 0.0).astype(bf16))
            xs = [x[w * rows_of : (w + 1) * rows_of] for x in xs for w in own]
            return acc + mm(jnp.concatenate(xs, 1), jnp.concatenate(matches, 0))

        def over(of_s, of_t, acc, between=()):
            step = functools.partial(one, of_s, of_t, between)
            return step(0, acc) if blocks == 1 else lax.fori_loop(0, blocks, step, acc)

        acc = over(sides(t_low, ra, 5), sides(s_low, rb, 4), jnp.zeros((rows_of, m), f32), between)
        again = lambda x: over(sides(t_high, ra, 5), sides(s_high, rb, 4), x)
        return acc, lambda x: lax.cond(more, again, lambda x: x, x)

    def factor(i, table):
        rows = lanes(i, 0)
        at = mm(table, one_hot(rows, 4))
        at = at[0:KEYS] + at[KEYS : 2 * KEYS] + at[2 * KEYS : 3 * KEYS]
        return jnp.sum(jnp.where(one_hot(rows, 5) > 0.5, at, 0.0), axis=0, keepdims=True)

    def finish(i, acc, by):
        acc = acc * by
        acc = jnp.concatenate([acc] * split_w, 0).T.reshape(srcs, cap, LANES)
        result = acc[:, 0:part]
        for w in range(1, split_w):
            lane = iota((srcs, part, LANES), 2)
            result = jnp.where(lane < w * rows_of, result, acc[:, w * part : (w + 1) * part])
        out[pl.ds(i * srcs, srcs)] = result

    if blocks == 1:
        kept = {}
        found = tables(own_counts(0))
        halves = halves_of(all_counts(0))
        between = {
            0: lambda: kept.update(table=scales(halves)),
            split_w: lambda: kept.update(by=factor(0, kept["table"])),
        }
        acc, rest = joins(0, *found, between)
        finish(0, rest(acc), kept["by"])
        return

    own_ref[...] = jnp.zeros_like(own_ref)
    all_ref[...] = jnp.zeros_like(all_ref)

    @pl.loop(0, blocks)
    def _(i):
        for k, (mine, every) in enumerate(zip(own_counts(i), all_counts(i))):
            own_ref[k] += mine
            all_ref[k] += every

    found, more = tables([own_ref[0], own_ref[1]])
    table = scales(halves_of([all_ref[0], all_ref[1]]))

    @pl.loop(0, blocks)
    def _(i):
        acc, rest = joins(i, found, more)
        finish(i, rest(acc), factor(i, table))


def body(sizes, r_rows, r_keys, r_counts, s_rows, s_keys, s_counts, t_rows, t_keys, t_counts):
    n_a, n_b, n_c = sizes
    n = n_a * n_b * n_c
    cap = r_keys.shape[0] // r_counts.shape[0]
    width = r_rows.shape[1]
    srcs = max(512 // cap, 1)
    srcs = srcs if n % srcs == 0 else n
    total_slots = n * cap
    split_w = 2 if n_c % 2 == 0 and width == LANES and cap % 16 == 0 else 1
    meta_rows = 8 if n_c * cap == LANES else 4
    assert n_c * cap in (LANES, LANES // 2) and n % (2 * n_c) == 0 and n * cap < BIG
    tiles = (2 * cap + meta_rows) // TILE
    row = lambda x: x.reshape(1, x.shape[0])
    far = lambda x: pltpu.with_memory_space_constraint(x, pltpu.HBM)
    near = lambda x: pltpu.with_memory_space_constraint(x, pltpu.VMEM)
    params = pltpu.CompilerParams(vmem_limit_bytes=40 << 20)
    small = (row(s_keys), row(t_keys), row(r_keys), row(s_counts), row(t_counts), row(r_counts))
    groups = (s_rows.shape[0] // cap, t_rows.shape[0] // cap, r_rows.shape[0] // cap)
    blocked = [x.reshape(g, cap, width) for x, g in zip((s_rows, t_rows, r_rows), groups)]
    near_like = lambda x: pltpu.VMEM(x.shape, x.dtype)
    packed, r_kept = pl.pallas_call(
        functools.partial(pack_kernel, n_a, n_b, n_c, cap, split_w),
        in_specs=[pl.BlockSpec(memory_space=pltpu.HBM)] * 9,
        out_shape=(pltpu.VMEM((n * tiles, TILE, width), bf16), near_like(blocked[2])),
        scratch_shapes=[near_like(x) for x in (*blocked[:2], *small)]
        + [pltpu.SemaphoreType.DMA((9,))],
        compiler_params=params,
        name="pack",
    )(*map(far, (*blocked, *small)))
    held = lax.all_to_all(packed, AXES, split_axis=0, concat_axis=0, tiled=True)
    shares = pl.pallas_call(
        functools.partial(join_kernel, n_c, cap, split_w, srcs, tiles),
        out_shape=pltpu.VMEM((n, cap // split_w, width), f32),
        scratch_shapes=[pltpu.VMEM((split_w, total_slots, LANES), bf16)] * 2
        + [
            pltpu.VMEM((2, split_w * KEYS, split_w * KEYS), f32),
            pltpu.VMEM((2, n_c * KEYS, n_c * KEYS), f32),
        ],
        compiler_params=params,
        name="join",
    )(near(held))
    back = lax.all_to_all(shares, AXES, split_axis=0, concat_axis=0, tiled=True)
    joined = pl.pallas_call(
        functools.partial(home_kernel, split_w),
        out_shape=jax.ShapeDtypeStruct(blocked[2].shape, bf16),
        compiler_params=params,
        name="home",
    )(near(back.reshape(n_a * n_b, n_c, cap // split_w, width)), near(r_kept))
    return joined.reshape(r_rows.shape)


def solution(mesh):
    rows, flat = P(AXES, None), P(AXES)
    sizes = tuple(mesh.shape[name] for name in AXES)
    return jax.shard_map(
        functools.partial(body, sizes),
        mesh=mesh,
        in_specs=(rows, flat, flat) * 3,
        out_specs=rows,
        check_vma=False,
    )
```

```python
import functools

import jax
import jax.numpy as jnp
from jax import lax
from jax.experimental import pallas as pl
from jax.experimental.pallas import tpu as pltpu
from jax.sharding import PartitionSpec as P

KEYS = 64
LANES = 128
TILE = 4
AXES = ("aa", "ba", "col")
f32 = jnp.float32
bf16 = jnp.bfloat16


def iota(shape, dim):
    return lax.broadcasted_iota(jnp.int32, shape, dim)


def split(x):
    hi = x.astype(bf16)
    return hi, (x - hi.astype(f32)).astype(bf16)


def mm(x, y):
    return lax.dot_general(x, y, (((1,), (0,)), ((), ())), preferred_element_type=f32)


def mm_nt(x, y):
    return lax.dot_general(x, y, (((1,), (1,)), ((), ())), preferred_element_type=f32)


def mm_tn(x, y):
    return lax.dot_general(x, y, (((0,), (0,)), ((), ())), preferred_element_type=f32)


def swap(x, y):
    half = x.shape[-1] // 2
    low = iota(x.shape, x.ndim - 1) < half
    turn = lambda v: pltpu.roll(v, half, v.ndim - 1)
    return jnp.where(low, x, turn(y)), jnp.where(low, turn(x), y)


def pack_kernel(
    n_a, n_b, n_c, cap, split_w,
    s_rows, t_rows, r_rows, s_keys, t_keys, r_keys, s_cnt, t_cnt, r_cnt,
    out, r_out,
    s_near, t_near,
    s_keys_near, t_keys_near, r_keys_near, s_cnt_near, t_cnt_near, r_cnt_near, sem,
):
    small = [
        pltpu.make_async_copy(far, near, sem.at[i])
        for i, (far, near) in enumerate(
            (
                (s_keys, s_keys_near),
                (t_keys, t_keys_near),
                (r_keys, r_keys_near),
                (s_cnt, s_cnt_near),
                (t_cnt, t_cnt_near),
                (r_cnt, r_cnt_near),
            )
        )
    ]
    rows = [
        pltpu.make_async_copy(far, near, sem.at[len(small) + i])
        for i, (far, near) in enumerate(((s_rows, s_near), (t_rows, t_near), (r_rows, r_out)))
    ]
    for copy in small + rows:
        copy.start()

    def halves(keys_ref, cnt_ref):
        keys = keys_ref[...]
        slots = keys.shape[1]
        groups = slots // cap
        spread = (iota((groups, slots), 1) // cap == iota((groups, slots), 0)).astype(bf16)
        cnt = jnp.broadcast_to(cnt_ref[...].astype(f32).astype(bf16), (8, groups))
        live = (iota((1, slots), 1) % cap).astype(f32) < mm(cnt, spread)[0:1]
        first = jnp.where(live, lax.div(keys, KEYS).astype(f32), -1.0)
        second = jnp.where(live, lax.rem(keys, KEYS).astype(f32), -1.0)
        return first, second

    def at(vec, start):
        row = vec[:, start // LANES * LANES : (start // LANES + 1) * LANES]
        return pltpu.roll(row, (LANES - start % LANES) % LANES, 1) if start % LANES else row

    for copy in small:
        copy.wait()
    sb, sc = halves(s_keys_near, s_cnt_near)
    ta, tc = halves(t_keys_near, t_cnt_near)
    ra, rb = halves(r_keys_near, r_cnt_near)
    seg = n_c * cap
    tiles = out.shape[0] // (n_a * n_b * n_c)
    meta_rows = tiles * TILE - 2 * cap
    row = iota((meta_rows, LANES), 0)
    lane = iota((1, LANES), 1)
    me = (lax.axis_index("aa") * n_b + lax.axis_index("ba")) * n_c + lax.axis_index("col")
    turn = lax.rem(me, n_c) * cap

    def put(d, start, value):
        for t in range(value.shape[0] // TILE):
            out[d * tiles + start // TILE + t] = value[t * TILE : (t + 1) * TILE]

    def pairs(first, second, start):
        first, second = at(first, start), at(second, start)
        if seg == LANES:
            return [first, second]
        return [jnp.where(lane < seg, first, pltpu.roll(second, seg, 1))]

    def repeated(first, second):
        slots = first.shape[1]
        groups = slots // cap
        mine = iota((groups, slots), 1) // cap == iota((groups, slots), 0)
        same = iota((slots, LANES), 0) % cap == iota((slots, LANES), 1) % cap
        low = iota((slots, LANES), 1) < seg
        spread = lambda x, to: mm(jnp.where(mine, x, 0.0).astype(bf16), to.astype(bf16))
        if seg == LANES:
            return [spread(first, same), spread(second, same)]
        return [spread(first, same & low) + spread(second, same & ~low)]

    def turned(meta, by):
        if seg == LANES:
            return pltpu.roll(meta, by, 1)
        return jnp.where(
            iota(meta.shape, 1) % seg >= by, pltpu.roll(meta, by, 1), pltpu.roll(meta, by + seg, 1)
        )

    s_meta = [pairs(sb, sc, b * seg) for b in range(n_b)]
    t_meta = [pairs(ta, tc, a * seg) for a in range(n_a)]
    r_meta = repeated(ra, rb)
    for a in range(n_a):
        for b in range(n_b):
            g = a * n_b + b
            meta = jnp.zeros((meta_rows, LANES), f32)
            for k, value in enumerate(s_meta[b] + t_meta[a] + [x[g : g + 1] for x in r_meta]):
                meta = jnp.where(row == k, value, meta)
            for c in range(0, n_c, split_w):
                part = turned(meta, lax.rem(turn + seg - c * cap, seg)).astype(bf16)
                for w in range(split_w):
                    put(g * n_c + c + w, 2 * cap, part)
    for copy in rows:
        copy.wait()

    def parts(near, g):
        if split_w == 1:
            return (near[g],)
        pair = swap(near[g].astype(f32), near[g + 1].astype(f32))
        return tuple(x.astype(bf16) for x in pair)

    for c in range(0, n_c, split_w):
        for b in range(n_b):
            for w, part in enumerate(parts(s_near, b * n_c + c)):
                for a in range(n_a):
                    put((a * n_b + b) * n_c + c + w, 0, part)
        for a in range(n_a):
            for w, part in enumerate(parts(t_near, a * n_c + c)):
                for b in range(n_b):
                    put((a * n_b + b) * n_c + c + w, cap, part)


def home_kernel(split_w, shares, r_rows, out):
    groups, n_c, cap_w, width = shares.shape
    total = [shares[:, w] for w in range(split_w)]
    for c in range(split_w, n_c):
        total[c % split_w] = total[c % split_w] + shares[:, c]
    if split_w == 2:
        total = swap(*total)
    for w in range(split_w):
        at = pl.ds(w * cap_w, cap_w)
        out[:, at, :] = (r_rows[:, at, :].astype(f32) * total[w]).astype(bf16)


EXACT = 256.0
SHIFT = 4096.0
ROUND = 1.5 * 2.0**23 * SHIFT


def join_kernel(n_c, cap, split_w, srcs, tiles, held, out, s_ref, t_ref, own_ref, all_ref):
    blocks = held.shape[0] // (srcs * tiles)
    m = srcs * cap
    seg = n_c * cap
    rows_of = LANES // split_w
    part = cap // split_w
    key = iota((KEYS, m), 0).astype(f32).astype(bf16)

    def block_of(i):
        return held[pl.ds(i * srcs * tiles, srcs * tiles)].reshape(srcs, tiles, TILE, LANES)

    def lanes(i, bucket):
        meta = block_of(i)[:, 2 * cap // TILE :].astype(f32)
        meta = meta.reshape(srcs, meta.shape[1] * TILE, LANES)
        block = iota(meta.shape[1:], 1) % seg // cap
        groups = []
        for g in range(0, srcs, n_c):
            row = meta[g]
            for j in range(1, n_c):
                row = jnp.where(block == (j + bucket) % n_c, meta[g + j], row)
            groups.append(row)
        if seg == LANES:
            rows = jnp.concatenate(groups, 1)
            return [rows[k : k + 1] for k in range(6)]
        low = iota(meta.shape[1:], 1) < seg
        swapped = [
            (jnp.where(low, x, pltpu.roll(y, seg, 1)), jnp.where(low, pltpu.roll(x, seg, 1), y))
            for x, y in zip(groups[0::2], groups[1::2])
        ]
        both = [jnp.concatenate(x, 1) for x in zip(*swapped)]
        return [both[k % 2][k // 2 : k // 2 + 1] for k in range(6)]

    def hot_of(rows, kind):
        return jnp.broadcast_to(rows[kind], (KEYS, m)).astype(bf16) == key

    def one_hot(rows, kind):
        return jnp.where(hot_of(rows, kind), jnp.ones_like(key), jnp.zeros_like(key))

    def stack(i, kind, buckets):
        return jnp.concatenate([one_hot(lanes(i, bucket), kind) for bucket in buckets], 0)

    own = range(split_w)

    def own_counts(i):
        counts = []
        for k, ref in enumerate((s_ref, t_ref)):
            first, c = stack(i, 2 * k, own), stack(i, 2 * k + 1, own)
            counts.append(mm_nt(c, first))
            ref[pl.ds(i * m, m), :] = jnp.concatenate([c, first], 0).T
        return counts

    def all_counts(i):
        every = range(n_c)
        return [mm_nt(stack(i, 2 * k, every), stack(i, 2 * k + 1, every)) for k in range(2)]

    def tables(own_found):
        found = []
        for count in own_found:
            same = iota(count.shape, 0) // KEYS == iota(count.shape, 1) // KEYS
            count = jnp.where(same, count, 0.0)
            high = jnp.floor(count / EXACT)
            found.append((count - EXACT * high, high))
        more = jnp.maximum(jnp.max(found[0][1]), jnp.max(found[1][1])) > 0.0
        return [(low.astype(bf16), high.astype(bf16)) for low, high in found], more

    def halves_of(all_found):
        halves = []
        for count in all_found:
            block = iota((KEYS, count.shape[1]), 1) // KEYS
            total = count[0:KEYS]
            for b in range(1, n_c):
                total = jnp.where(block == b, count[b * KEYS : (b + 1) * KEYS], total)
            halves.append(split(total))
        return halves

    def scales(halves):
        triangles = sum(mm_nt(s, t) for s in halves[0] for t in halves[1])
        scale = 1.0 / jnp.sqrt(1.0 + triangles)
        hi, _ = split(scale)
        middle, rest = split(scale - hi.astype(f32))
        return jnp.concatenate([hi, middle, rest], 0)

    def joins(i, found, more, between=()):
        rows = lanes(i, 0)
        ra, rb = [jnp.concatenate([one_hot(rows, k)] * split_w, 0) for k in (4, 5)]
        (s_low, s_high), (t_low, t_high) = found

        def side(table, hot, kind_flag):
            value = mm(table, hot)
            flag = lambda w: jnp.where(
                hot_of(rows, kind_flag), jnp.zeros_like(key), jnp.full_like(key, -2 * EXACT * SHIFT**w)
            )
            value = [(value[w * KEYS : (w + 1) * KEYS] * SHIFT**w).astype(bf16) for w in own]
            return jnp.concatenate(value + [flag(w) for w in own], 0)

        def one(of_s, of_t, between, j, accs):
            at = pl.ds(j * m, m)
            rows = block_of(j)
            xs, matches = [], [[] for _ in own]
            for left, ref, start in ((of_s, s_ref, 0), (of_t, t_ref, cap)):
                x = rows[:, start // TILE : (start + cap) // TILE]
                x = x.reshape(srcs // n_c, n_c, cap, LANES)
                turned = x.reshape(m, LANES)
                for w in range(1, split_w):
                    shifted = jnp.concatenate([x[:, n_c - w :], x[:, : n_c - w]], 1).reshape(m, LANES)
                    turned = jnp.concatenate([turned[:, : w * rows_of], shifted[:, w * rows_of :]], 1)
                xs.append(turned.T)
                if len(xs) in between:
                    between[len(xs)]()
                both = mm(ref[at], left)
                if split_w == 2:
                    second = (both + ROUND) - ROUND
                    both = (both - second, second)
                else:
                    both = (both,)
                for w in own:
                    matches[w].append(jnp.maximum(both[w].astype(bf16), jnp.zeros((), bf16)))
            return tuple(
                acc
                + mm(
                    jnp.concatenate([x[w * rows_of : (w + 1) * rows_of] for x in xs], 1),
                    jnp.concatenate(matches[w], 0),
                )
                for w, acc in enumerate(accs)
            )

        def over(of_s, of_t, between=()):
            step = functools.partial(one, of_s, of_t, between)
            accs = tuple(jnp.zeros((rows_of, m), f32) for _ in own)
            accs = step(0, accs) if blocks == 1 else lax.fori_loop(0, blocks, step, accs)
            return sum(acc * SHIFT**-w for w, acc in enumerate(accs))

        acc = over(side(t_low, ra, 5), side(s_low, rb, 4), between)
        again = lambda x: x + EXACT * over(side(t_high, ra, 5), side(s_high, rb, 4))
        return acc, lambda x: lax.cond(more, again, lambda x: x, x)

    def factor(i, table):
        rows = lanes(i, 0)
        at = mm(table, one_hot(rows, 4))
        at = at[0:KEYS] + at[KEYS : 2 * KEYS] + at[2 * KEYS : 3 * KEYS]
        return jnp.sum(jnp.where(one_hot(rows, 5) > 0.5, at, 0.0), axis=0, keepdims=True)

    def finish(i, acc, by):
        acc = acc * by
        acc = jnp.concatenate([acc] * split_w, 0).T.reshape(srcs, cap, LANES)
        result = acc[:, 0:part]
        for w in range(1, split_w):
            lane = iota((srcs, part, LANES), 2)
            result = jnp.where(lane < w * rows_of, result, acc[:, w * part : (w + 1) * part])
        out[pl.ds(i * srcs, srcs)] = result

    if blocks == 1:
        kept = {}
        found = tables(own_counts(0))
        halves = halves_of(all_counts(0))
        between = {
            1: lambda: kept.update(table=scales(halves)),
            2: lambda: kept.update(by=factor(0, kept["table"])),
        }
        acc, rest = joins(0, *found, between)
        finish(0, rest(acc), kept["by"])
        return

    own_ref[...] = jnp.zeros_like(own_ref)
    all_ref[...] = jnp.zeros_like(all_ref)

    @pl.loop(0, blocks)
    def _(i):
        for k, (mine, every) in enumerate(zip(own_counts(i), all_counts(i))):
            own_ref[k] += mine
            all_ref[k] += every

    found, more = tables([own_ref[0], own_ref[1]])
    table = scales(halves_of([all_ref[0], all_ref[1]]))

    @pl.loop(0, blocks)
    def _(i):
        acc, rest = joins(i, found, more)
        finish(i, rest(acc), factor(i, table))


def body(sizes, r_rows, r_keys, r_counts, s_rows, s_keys, s_counts, t_rows, t_keys, t_counts):
    n_a, n_b, n_c = sizes
    n = n_a * n_b * n_c
    cap = r_keys.shape[0] // r_counts.shape[0]
    width = r_rows.shape[1]
    srcs = max(512 // cap, 1)
    srcs = srcs if n % srcs == 0 else n
    total_slots = n * cap
    split_w = 2 if n_c % 2 == 0 and width == LANES and cap % 16 == 0 else 1
    meta_rows = 8 if n_c * cap == LANES else 4
    assert n_c * cap in (LANES, LANES // 2) and n % (2 * n_c) == 0 and n * cap < EXACT**2
    tiles = (2 * cap + meta_rows) // TILE
    row = lambda x: x.reshape(1, x.shape[0])
    far = lambda x: pltpu.with_memory_space_constraint(x, pltpu.HBM)
    near = lambda x: pltpu.with_memory_space_constraint(x, pltpu.VMEM)
    params = pltpu.CompilerParams(vmem_limit_bytes=40 << 20)
    small = (row(s_keys), row(t_keys), row(r_keys), row(s_counts), row(t_counts), row(r_counts))
    groups = (s_rows.shape[0] // cap, t_rows.shape[0] // cap, r_rows.shape[0] // cap)
    blocked = [x.reshape(g, cap, width) for x, g in zip((s_rows, t_rows, r_rows), groups)]
    near_like = lambda x: pltpu.VMEM(x.shape, x.dtype)
    packed, r_kept = pl.pallas_call(
        functools.partial(pack_kernel, n_a, n_b, n_c, cap, split_w),
        in_specs=[pl.BlockSpec(memory_space=pltpu.HBM)] * 9,
        out_shape=(pltpu.VMEM((n * tiles, TILE, width), bf16), near_like(blocked[2])),
        scratch_shapes=[near_like(x) for x in (*blocked[:2], *small)]
        + [pltpu.SemaphoreType.DMA((9,))],
        compiler_params=params,
        name="pack",
    )(*map(far, (*blocked, *small)))
    held = lax.all_to_all(packed, AXES, split_axis=0, concat_axis=0, tiled=True)
    shares = pl.pallas_call(
        functools.partial(join_kernel, n_c, cap, split_w, srcs, tiles),
        out_shape=pltpu.VMEM((n, cap // split_w, width), f32),
        scratch_shapes=[pltpu.VMEM((total_slots, 2 * split_w * KEYS), bf16)] * 2
        + [
            pltpu.VMEM((2, split_w * KEYS, split_w * KEYS), f32),
            pltpu.VMEM((2, n_c * KEYS, n_c * KEYS), f32),
        ],
        compiler_params=params,
        name="join",
    )(near(held))
    back = lax.all_to_all(shares, AXES, split_axis=0, concat_axis=0, tiled=True)
    joined = pl.pallas_call(
        functools.partial(home_kernel, split_w),
        out_shape=jax.ShapeDtypeStruct(blocked[2].shape, bf16),
        compiler_params=params,
        name="home",
    )(near(back.reshape(n_a * n_b, n_c, cap // split_w, width)), near(r_kept))
    return joined.reshape(r_rows.shape)


def solution(mesh):
    rows, flat = P(AXES, None), P(AXES)
    sizes = tuple(mesh.shape[name] for name in AXES)
    return jax.shard_map(
        functools.partial(body, sizes),
        mesh=mesh,
        in_specs=(rows, flat, flat) * 3,
        out_specs=rows,
        check_vma=False,
    )
```

```python
import functools

import jax
import jax.numpy as jnp
from jax import lax
from jax.experimental import pallas as pl
from jax.experimental.pallas import tpu as pltpu
from jax.sharding import PartitionSpec as P

KEYS = 64
LANES = 128
TILE = 4
AXES = ("aa", "ba", "col")
f32 = jnp.float32
bf16 = jnp.bfloat16


def iota(shape, dim):
    return lax.broadcasted_iota(jnp.int32, shape, dim)


def split(x):
    hi = x.astype(bf16)
    return hi, (x - hi.astype(f32)).astype(bf16)


def mm(x, y):
    return lax.dot_general(x, y, (((1,), (0,)), ((), ())), preferred_element_type=f32)


def mm_nt(x, y):
    return lax.dot_general(x, y, (((1,), (1,)), ((), ())), preferred_element_type=f32)


def mm_tn(x, y):
    return lax.dot_general(x, y, (((0,), (0,)), ((), ())), preferred_element_type=f32)


def swap(x, y):
    half = x.shape[-1] // 2
    low = iota(x.shape, x.ndim - 1) < half
    turn = lambda v: pltpu.roll(v, half, v.ndim - 1)
    return jnp.where(low, x, turn(y)), jnp.where(low, turn(x), y)


def pack_kernel(
    n_a, n_b, n_c, cap, split_w,
    s_rows, t_rows, r_rows, s_keys, t_keys, r_keys, s_cnt, t_cnt, r_cnt,
    out, r_out,
    s_near, t_near,
    s_keys_near, t_keys_near, r_keys_near, s_cnt_near, t_cnt_near, r_cnt_near, sem,
):
    small = [
        pltpu.make_async_copy(far, near, sem.at[i])
        for i, (far, near) in enumerate(
            (
                (s_keys, s_keys_near),
                (t_keys, t_keys_near),
                (r_keys, r_keys_near),
                (s_cnt, s_cnt_near),
                (t_cnt, t_cnt_near),
                (r_cnt, r_cnt_near),
            )
        )
    ]
    rows = [
        pltpu.make_async_copy(far, near, sem.at[len(small) + i])
        for i, (far, near) in enumerate(((s_rows, s_near), (t_rows, t_near), (r_rows, r_out)))
    ]
    for copy in small + rows:
        copy.start()

    def halves(keys_ref, cnt_ref):
        keys = keys_ref[...]
        slots = keys.shape[1]
        groups = slots // cap
        spread = (iota((groups, slots), 1) // cap == iota((groups, slots), 0)).astype(bf16)
        cnt = jnp.broadcast_to(cnt_ref[...].astype(f32).astype(bf16), (8, groups))
        live = (iota((1, slots), 1) % cap).astype(f32) < mm(cnt, spread)[0:1]
        keys = keys.astype(f32)
        high = jnp.floor(keys * (1.0 / KEYS))
        first = jnp.where(live, high, -1.0)
        second = jnp.where(live, keys - KEYS * high, -1.0)
        return first, second

    def at(vec, start):
        row = vec[:, start // LANES * LANES : (start // LANES + 1) * LANES]
        return pltpu.roll(row, (LANES - start % LANES) % LANES, 1) if start % LANES else row

    for copy in small:
        copy.wait()
    sb, sc = halves(s_keys_near, s_cnt_near)
    ta, tc = halves(t_keys_near, t_cnt_near)
    ra, rb = halves(r_keys_near, r_cnt_near)
    seg = n_c * cap
    tiles = out.shape[0] // (n_a * n_b * n_c)
    meta_rows = tiles * TILE - 2 * cap
    row = iota((meta_rows, LANES), 0)
    lane = iota((1, LANES), 1)
    me = (lax.axis_index("aa") * n_b + lax.axis_index("ba")) * n_c + lax.axis_index("col")
    turn = lax.rem(me, n_c) * cap

    def put(d, start, value):
        for t in range(value.shape[0] // TILE):
            out[d * tiles + start // TILE + t] = value[t * TILE : (t + 1) * TILE]

    def pairs(first, second, start):
        first, second = at(first, start), at(second, start)
        if seg == LANES:
            return [first, second]
        return [jnp.where(lane < seg, first, pltpu.roll(second, seg, 1))]

    def repeated(first, second):
        slots = first.shape[1]
        groups = slots // cap
        mine = iota((groups, slots), 1) // cap == iota((groups, slots), 0)
        same = iota((slots, LANES), 0) % cap == iota((slots, LANES), 1) % cap
        low = iota((slots, LANES), 1) < seg
        spread = lambda x, to: mm(jnp.where(mine, x, 0.0).astype(bf16), to.astype(bf16))
        if seg == LANES:
            return [spread(first, same), spread(second, same)]
        return [spread(first, same & low) + spread(second, same & ~low)]

    def turned(meta, by):
        if seg == LANES:
            return pltpu.roll(meta, by, 1)
        return jnp.where(
            iota(meta.shape, 1) % seg >= by, pltpu.roll(meta, by, 1), pltpu.roll(meta, by + seg, 1)
        )

    s_meta = [pairs(sb, sc, b * seg) for b in range(n_b)]
    t_meta = [pairs(ta, tc, a * seg) for a in range(n_a)]
    r_meta = repeated(ra, rb)
    for a in range(n_a):
        for b in range(n_b):
            g = a * n_b + b
            meta = jnp.zeros((meta_rows, LANES), f32)
            for k, value in enumerate(s_meta[b] + t_meta[a] + [x[g : g + 1] for x in r_meta]):
                meta = jnp.where(row == k, value, meta)
            for c in range(0, n_c, split_w):
                part = turned(meta, lax.rem(turn + seg - c * cap, seg)).astype(bf16)
                for w in range(split_w):
                    put(g * n_c + c + w, 2 * cap, part)
    for copy in rows:
        copy.wait()

    def parts(near, g):
        if split_w == 1:
            return (near[g],)
        pair = swap(near[g].astype(f32), near[g + 1].astype(f32))
        return tuple(x.astype(bf16) for x in pair)

    for c in range(0, n_c, split_w):
        for b in range(n_b):
            for w, part in enumerate(parts(s_near, b * n_c + c)):
                for a in range(n_a):
                    put((a * n_b + b) * n_c + c + w, 0, part)
        for a in range(n_a):
            for w, part in enumerate(parts(t_near, a * n_c + c)):
                for b in range(n_b):
                    put((a * n_b + b) * n_c + c + w, cap, part)


def home_kernel(split_w, shares, r_rows, out):
    groups, n_c, cap_w, width = shares.shape
    total = [shares[:, w] for w in range(split_w)]
    for c in range(split_w, n_c):
        total[c % split_w] = total[c % split_w] + shares[:, c]
    if split_w == 2:
        total = swap(*total)
    for w in range(split_w):
        at = pl.ds(w * cap_w, cap_w)
        out[:, at, :] = (r_rows[:, at, :].astype(f32) * total[w]).astype(bf16)


EXACT = 256.0
SHIFT = 4096.0
ROUND = 1.5 * 2.0**23 * SHIFT


def join_kernel(n_c, cap, split_w, srcs, tiles, held, out, s_ref, t_ref, own_ref, all_ref):
    blocks = held.shape[0] // (srcs * tiles)
    m = srcs * cap
    seg = n_c * cap
    rows_of = LANES // split_w
    part = cap // split_w
    key = iota((KEYS, m), 0).astype(f32).astype(bf16)

    def block_of(i):
        return held[pl.ds(i * srcs * tiles, srcs * tiles)].reshape(srcs, tiles, TILE, LANES)

    def lanes(i, bucket):
        meta = block_of(i)[:, 2 * cap // TILE :].astype(f32)
        meta = meta.reshape(srcs, meta.shape[1] * TILE, LANES)
        block = iota(meta.shape[1:], 1) % seg // cap
        groups = []
        for g in range(0, srcs, n_c):
            row = meta[g]
            for j in range(1, n_c):
                row = jnp.where(block == (j + bucket) % n_c, meta[g + j], row)
            groups.append(row)
        if seg == LANES:
            rows = jnp.concatenate(groups, 1)
            return [rows[k : k + 1] for k in range(6)]
        low = iota(meta.shape[1:], 1) < seg
        swapped = [
            (jnp.where(low, x, pltpu.roll(y, seg, 1)), jnp.where(low, pltpu.roll(x, seg, 1), y))
            for x, y in zip(groups[0::2], groups[1::2])
        ]
        both = [jnp.concatenate(x, 1) for x in zip(*swapped)]
        return [both[k % 2][k // 2 : k // 2 + 1] for k in range(6)]

    def hot_of(rows, kind):
        return jnp.broadcast_to(rows[kind], (KEYS, m)).astype(bf16) == key

    def one_hot(rows, kind):
        return jnp.where(hot_of(rows, kind), jnp.ones_like(key), jnp.zeros_like(key))

    def stack(i, kind, buckets):
        return jnp.concatenate([one_hot(lanes(i, bucket), kind) for bucket in buckets], 0)

    own = range(split_w)

    def own_counts(i):
        counts = []
        for k, ref in enumerate((s_ref, t_ref)):
            first, c = stack(i, 2 * k, own), stack(i, 2 * k + 1, own)
            counts.append(mm_nt(c, first))
            ref[pl.ds(i * m, m), :] = jnp.concatenate([c, first], 0).T
        return counts

    def all_counts(i):
        every = range(n_c)
        return [mm_nt(stack(i, 2 * k, every), stack(i, 2 * k + 1, every)) for k in range(2)]

    def tables(own_found):
        found = []
        for count in own_found:
            same = iota(count.shape, 0) // KEYS == iota(count.shape, 1) // KEYS
            count = jnp.where(same, count, 0.0)
            high = jnp.floor(count / EXACT)
            found.append((count - EXACT * high, high))
        more = jnp.maximum(jnp.max(found[0][1]), jnp.max(found[1][1])) > 0.0
        return [(low.astype(bf16), high.astype(bf16)) for low, high in found], more

    def halves_of(all_found):
        halves = []
        for count in all_found:
            block = iota((KEYS, count.shape[1]), 1) // KEYS
            total = count[0:KEYS]
            for b in range(1, n_c):
                total = jnp.where(block == b, count[b * KEYS : (b + 1) * KEYS], total)
            halves.append(split(total))
        return halves

    def scales(halves):
        triangles = sum(mm_nt(s, t) for s in halves[0] for t in halves[1])
        scale = 1.0 / jnp.sqrt(1.0 + triangles)
        hi, _ = split(scale)
        middle, rest = split(scale - hi.astype(f32))
        return jnp.concatenate([hi, middle, rest], 0)

    def joins(i, found, more, between=()):
        rows = lanes(i, 0)
        ra, rb = [jnp.concatenate([one_hot(rows, k)] * split_w, 0) for k in (4, 5)]
        (s_low, s_high), (t_low, t_high) = found

        def side(table, hot, kind_flag):
            value = mm(table, hot)
            flag = lambda w: jnp.where(
                hot_of(rows, kind_flag), jnp.zeros_like(key), jnp.full_like(key, -2 * EXACT * SHIFT**w)
            )
            value = [(value[w * KEYS : (w + 1) * KEYS] * SHIFT**w).astype(bf16) for w in own]
            return jnp.concatenate(value + [flag(w) for w in own], 0)

        def one(of_s, of_t, between, j, accs):
            at = pl.ds(j * m, m)
            rows = block_of(j)
            xs, matches = [], [[] for _ in own]
            for left, ref, start in ((of_s, s_ref, 0), (of_t, t_ref, cap)):
                x = rows[:, start // TILE : (start + cap) // TILE]
                x = x.reshape(srcs // n_c, n_c, cap, LANES)
                turned = x.reshape(m, LANES)
                for w in range(1, split_w):
                    shifted = jnp.concatenate([x[:, n_c - w :], x[:, : n_c - w]], 1).reshape(m, LANES)
                    turned = jnp.concatenate([turned[:, : w * rows_of], shifted[:, w * rows_of :]], 1)
                xs.append(turned.T)
                if len(xs) in between:
                    between[len(xs)]()
                both = mm(ref[at], left)
                if split_w == 2:
                    second = (both + ROUND) - ROUND
                    both = (both - second, second)
                else:
                    both = (both,)
                for w in own:
                    matches[w].append(jnp.maximum(both[w].astype(bf16), jnp.zeros((), bf16)))
            return tuple(
                acc
                + mm(
                    jnp.concatenate([x[w * rows_of : (w + 1) * rows_of] for x in xs], 1),
                    jnp.concatenate(matches[w], 0),
                )
                for w, acc in enumerate(accs)
            )

        def over(of_s, of_t, between=()):
            step = functools.partial(one, of_s, of_t, between)
            accs = tuple(jnp.zeros((rows_of, m), f32) for _ in own)
            accs = step(0, accs) if blocks == 1 else lax.fori_loop(0, blocks, step, accs)
            return sum(acc * SHIFT**-w for w, acc in enumerate(accs))

        acc = over(side(t_low, ra, 5), side(s_low, rb, 4), between)
        again = lambda x: x + EXACT * over(side(t_high, ra, 5), side(s_high, rb, 4))
        return acc, lambda x: lax.cond(more, again, lambda x: x, x)

    def factor(i, table):
        rows = lanes(i, 0)
        at = mm(table, one_hot(rows, 4))
        at = at[0:KEYS] + at[KEYS : 2 * KEYS] + at[2 * KEYS : 3 * KEYS]
        return jnp.sum(jnp.where(one_hot(rows, 5) > 0.5, at, 0.0), axis=0, keepdims=True)

    def finish(i, acc, by):
        acc = acc * by
        acc = jnp.concatenate([acc] * split_w, 0).T.reshape(srcs, cap, LANES)
        result = acc[:, 0:part]
        for w in range(1, split_w):
            lane = iota((srcs, part, LANES), 2)
            result = jnp.where(lane < w * rows_of, result, acc[:, w * part : (w + 1) * part])
        out[pl.ds(i * srcs, srcs)] = result

    if blocks == 1:
        kept = {}
        found = tables(own_counts(0))
        halves = halves_of(all_counts(0))
        between = {
            1: lambda: kept.update(table=scales(halves)),
            2: lambda: kept.update(by=factor(0, kept["table"])),
        }
        acc, rest = joins(0, *found, between)
        finish(0, rest(acc), kept["by"])
        return

    own_ref[...] = jnp.zeros_like(own_ref)
    all_ref[...] = jnp.zeros_like(all_ref)

    @pl.loop(0, blocks)
    def _(i):
        for k, (mine, every) in enumerate(zip(own_counts(i), all_counts(i))):
            own_ref[k] += mine
            all_ref[k] += every

    found, more = tables([own_ref[0], own_ref[1]])
    table = scales(halves_of([all_ref[0], all_ref[1]]))

    @pl.loop(0, blocks)
    def _(i):
        acc, rest = joins(i, found, more)
        finish(i, rest(acc), factor(i, table))


def body(sizes, r_rows, r_keys, r_counts, s_rows, s_keys, s_counts, t_rows, t_keys, t_counts):
    n_a, n_b, n_c = sizes
    n = n_a * n_b * n_c
    cap = r_keys.shape[0] // r_counts.shape[0]
    width = r_rows.shape[1]
    srcs = max(512 // cap, 1)
    srcs = srcs if n % srcs == 0 else n
    total_slots = n * cap
    split_w = 2 if n_c % 2 == 0 and width == LANES and cap % 16 == 0 else 1
    meta_rows = 8 if n_c * cap == LANES else 4
    assert n_c * cap in (LANES, LANES // 2) and n % (2 * n_c) == 0 and n * cap < EXACT**2
    tiles = (2 * cap + meta_rows) // TILE
    row = lambda x: x.reshape(1, x.shape[0])
    far = lambda x: pltpu.with_memory_space_constraint(x, pltpu.HBM)
    near = lambda x: pltpu.with_memory_space_constraint(x, pltpu.VMEM)
    params = pltpu.CompilerParams(vmem_limit_bytes=40 << 20)
    small = (row(s_keys), row(t_keys), row(r_keys), row(s_counts), row(t_counts), row(r_counts))
    groups = (s_rows.shape[0] // cap, t_rows.shape[0] // cap, r_rows.shape[0] // cap)
    blocked = [x.reshape(g, cap, width) for x, g in zip((s_rows, t_rows, r_rows), groups)]
    near_like = lambda x: pltpu.VMEM(x.shape, x.dtype)
    packed, r_kept = pl.pallas_call(
        functools.partial(pack_kernel, n_a, n_b, n_c, cap, split_w),
        in_specs=[pl.BlockSpec(memory_space=pltpu.HBM)] * 9,
        out_shape=(pltpu.VMEM((n * tiles, TILE, width), bf16), near_like(blocked[2])),
        scratch_shapes=[near_like(x) for x in (*blocked[:2], *small)]
        + [pltpu.SemaphoreType.DMA((9,))],
        compiler_params=params,
        name="pack",
    )(*map(far, (*blocked, *small)))
    held = lax.all_to_all(packed, AXES, split_axis=0, concat_axis=0, tiled=True)
    shares = pl.pallas_call(
        functools.partial(join_kernel, n_c, cap, split_w, srcs, tiles),
        out_shape=pltpu.VMEM((n, cap // split_w, width), f32),
        scratch_shapes=[pltpu.VMEM((total_slots, 2 * split_w * KEYS), bf16)] * 2
        + [
            pltpu.VMEM((2, split_w * KEYS, split_w * KEYS), f32),
            pltpu.VMEM((2, n_c * KEYS, n_c * KEYS), f32),
        ],
        compiler_params=params,
        name="join",
    )(near(held))
    back = lax.all_to_all(shares, AXES, split_axis=0, concat_axis=0, tiled=True)
    joined = pl.pallas_call(
        functools.partial(home_kernel, split_w),
        out_shape=jax.ShapeDtypeStruct(blocked[2].shape, bf16),
        compiler_params=params,
        name="home",
    )(near(back.reshape(n_a * n_b, n_c, cap // split_w, width)), near(r_kept))
    return joined.reshape(r_rows.shape)


def solution(mesh):
    rows, flat = P(AXES, None), P(AXES)
    sizes = tuple(mesh.shape[name] for name in AXES)
    return jax.shard_map(
        functools.partial(body, sizes),
        mesh=mesh,
        in_specs=(rows, flat, flat) * 3,
        out_specs=rows,
        check_vma=False,
    )
```
